256 devices in a mesh: section: 16 (over y, z_hi, core), rep: 4 (over z_lo), sub: 4 (over x).
Axes of the slice: x: 4, y: 4, z: 8 (z_hi: 2, z_lo: 4; z = z_hi * 4 + z_lo), core: 2. Of those that a mesh axis runs over, the one named last changes fastest.
Arguments:
- token_ids: int32 [8, 512], P(None, ('rep', 'sub')), may hold values from 0 to 255
- target_ids: int32 [8, 512], P(None, ('rep', 'sub')), may hold values from 0 to 255
- embedding: bfloat16 [256, 2048], P(('rep', 'sub')), may hold values from -3 to 3
- section_weight: bfloat16 [16, 2048, 2048], P('section', ('rep', 'sub')), may hold values from -0.125 to 0.125
- section_gain: float32 [16, 2048], P('section'), may hold values from 0.1 to 1.9
- final_gain: float32 [2048], replicated, may hold values from 0.5 to 1.5
Outputs:
- weight_grad: float32 [16, 2048, 2048], P('section', ('rep', 'sub'))
- gain_grad: float32 [16, 2048], P('section')
- embed_grad: float32 [256, 2048], P(('section', 'rep', 'sub'))
- final_grad: float32 [2048], replicated
The draws below stay inside these ranges and needn't reach their ends.
All inputs are finite; a program needn't handle non-finite values.
Results may differ from the reference program's by a relative error of at most 0.024.
Values may be sent and summed in bfloat16 or wider, within the bound.
No kernel may reach another device: no remote copies, remote signals or barrier semaphores. Data moves between devices by JAX's collectives and lax.ppermute only.
A program may use at most 64 MiB of HBM per device.

```python
import math
import jax
import jax.numpy as jnp
import numpy as np
from jax import lax

D = 2048
VOCAB = 256
MICRO = 8
SECTIONS = 16
TOKENS = 512
N_SECTION = 16


def set_ends(entries, key, low, largest):
    index_at = [jax.random.randint(jax.random.fold_in(key, axis), (), 0, length) for axis, length in enumerate(entries.shape)]
    main_axis = entries.shape.index(max(entries.shape))
    neighbour = index_at[:main_axis] + [(index_at[main_axis] + 1) % entries.shape[main_axis]] + index_at[main_axis + 1:]
    return entries.at[tuple(index_at)].set(low).at[tuple(neighbour)].set(largest)


def block_levels(key, extent, pieces, low, top_value):
    level = 1.0
    for axis_at, shards_of in pieces:
        draws = jax.random.uniform(jax.random.fold_in(jax.random.fold_in(key, 6), axis_at), (shards_of,), jnp.float32, low / len(pieces), top_value / len(pieces))
        level = level * jnp.repeat(jnp.exp(draws), extent[axis_at] // shards_of).reshape((-1,) + (1,) * (len(extent) - 1 - axis_at))
    return level


def cumulative_ranks(amount, slope):
    portions = [(1 << 20) // math.isqrt(grade ** slope) + 1 for grade in range(1, amount + 1)]
    width = 1 + sum(portions) // (1 << 30)
    return np.cumsum(np.array([max(1, weight // width) for weight in portions]))


def ranked(own_key, extent, count, lean):
    grid = cumulative_ranks(count, lean)
    pick = jax.random.randint(jax.random.fold_in(own_key, 1), extent, 0, int(grid[count - 1]))
    rank = jnp.searchsorted(jnp.asarray(grid, jnp.int32), pick, side="right")
    return jax.random.permutation(jax.random.fold_in(own_key, 2), count)[rank].astype(jnp.int32)


def centred(rng, shape, spread, most, split=(), kind=jnp.bfloat16):
    drawn = spread * jax.random.normal(rng, shape, jnp.float32)
    if split:
        drawn = drawn * block_levels(rng, shape, split, -0.22, 0.18)
    return jnp.clip(drawn, -most, most).astype(kind)


def setup_inputs(seed: int = 0) -> dict:
    key_list = jax.random.split(jax.random.key(seed), 7)
    return {
        "token_ids": set_ends(ranked(key_list[0], (MICRO, TOKENS), VOCAB, 2), jax.random.fold_in(key_list[0], 3), 0, VOCAB - 1).astype(jnp.int32),
        "target_ids": set_ends(ranked(key_list[1], (MICRO, TOKENS), VOCAB, 1), jax.random.fold_in(key_list[1], 3), 0, VOCAB - 1).astype(jnp.int32),
        "embedding": centred(key_list[2], (VOCAB, D), 0.25, 3.0, ((0, 16),)),
        "section_weight": centred(key_list[3], (SECTIONS, D, D), D ** -0.5, 0.125, ((0, 16), (1, 16))),
        "section_gain": jnp.clip(1.0 + 0.18 * jax.random.normal(key_list[4], (SECTIONS, D), jnp.float32), 0.1, 1.9),
        "final_gain": jnp.clip(1.0 + 0.1 * jax.random.normal(key_list[5], (D,), jnp.float32), 0.5, 1.5),
    }


epsilon = 1e-06
gelu_coef = 0.7978845608028654
cube_coef = 0.044715

def gelu(pre_act):
    return 0.5 * pre_act * (1.0 + jnp.tanh(gelu_coef * (pre_act + cube_coef * pre_act * pre_act * pre_act)))

def gelu_slope(pre_act):
    inside = gelu_coef * (pre_act + cube_coef * pre_act * pre_act * pre_act)
    tangent = jnp.tanh(inside)
    return 0.5 * (1.0 + tangent) + 0.5 * pre_act * (1.0 - tangent * tangent) * gelu_coef * (1.0 + 3.0 * cube_coef * pre_act * pre_act)

def normalize(residual, gain_row):
    values = residual.astype(jnp.float32)
    scale_inv = lax.rsqrt(lax.optimization_barrier(jnp.mean(values * values, axis=-1, keepdims=True)) + epsilon)
    normed = values * scale_inv
    return (normed, scale_inv, (normed * gain_row).astype(jnp.bfloat16))

def norm_back(grad_norm, normed, scale_inv, gain_row):
    grad_unit = grad_norm * gain_row
    grad_in = scale_inv * (grad_unit - normed * lax.optimization_barrier(jnp.mean(grad_unit * normed, axis=-1, keepdims=True)))
    return (grad_in, lax.optimization_barrier(jnp.sum(grad_norm * normed, axis=0)))

def reference(token_ids, target_ids, embedding, section_weight, section_gain, final_gain):
    vocab_iota = jnp.arange(VOCAB, dtype=jnp.int32)
    onehot_in = (token_ids.reshape(-1)[:, None] == vocab_iota[None, :]).astype(jnp.bfloat16)
    residual = jnp.dot(onehot_in, embedding, preferred_element_type=jnp.float32).astype(jnp.bfloat16)
    saved = []
    for layer_index in range(N_SECTION):
        normed, scale_inv, rounded = normalize(residual, section_gain[layer_index])
        pre_act = jnp.dot(rounded, section_weight[layer_index], preferred_element_type=jnp.float32)
        saved.append((residual, rounded, pre_act))
        residual = (residual.astype(jnp.float32) + gelu(pre_act)).astype(jnp.bfloat16)
    normed, scale_inv, final_rows = normalize(residual, final_gain)
    logit_scale = float(D) ** (-0.5)
    contract_last = (((1,), (1,)), ((), ()))
    contract_first = (((0,), (0,)), ((), ()))
    logits = lax.dot_general(final_rows, embedding, contract_last, preferred_element_type=jnp.float32) * logit_scale
    exp_logit = jnp.exp(logits)
    probability = exp_logit / lax.optimization_barrier(jnp.sum(exp_logit, axis=-1, keepdims=True))
    onehot_out = (target_ids.reshape(-1)[:, None] == vocab_iota[None, :]).astype(jnp.float32)
    grad_logit = ((probability - onehot_out) * logit_scale).astype(jnp.bfloat16)
    embed_head = lax.dot_general(grad_logit, final_rows, contract_first, preferred_element_type=jnp.float32)
    grad_final = jnp.dot(grad_logit, embedding, preferred_element_type=jnp.float32)
    grad_in, final_grad = norm_back(grad_final, normed, scale_inv, final_gain)
    grad_residual = grad_in.astype(jnp.bfloat16)
    weight_list = []
    gain_list = []
    for layer_index in reversed(range(N_SECTION)):
        residual_in, rounded, pre_act = saved[layer_index]
        grad_float = grad_residual.astype(jnp.float32)
        grad_pre = (grad_float * gelu_slope(pre_act)).astype(jnp.bfloat16)
        weight_list.append(lax.dot_general(rounded, grad_pre, contract_first, preferred_element_type=jnp.float32))
        grad_norm = lax.dot_general(grad_pre, section_weight[layer_index], contract_last, preferred_element_type=jnp.float32)
        normed, scale_inv, rounded_again = normalize(residual_in, section_gain[layer_index])
        grad_in, gain_part = norm_back(grad_norm, normed, scale_inv, section_gain[layer_index])
        gain_list.append(gain_part)
        grad_residual = (grad_float + grad_in).astype(jnp.bfloat16)
    embed_in = lax.dot_general(onehot_in, grad_residual, contract_first, preferred_element_type=jnp.float32)
    weight_grad = jnp.stack(weight_list[::-1])
    gain_grad = jnp.stack(gain_list[::-1])
    return (weight_grad, gain_grad, embed_in + embed_head, final_grad)
```

```python
import functools

import jax
import jax.numpy as jnp
from jax import lax
from jax.experimental import pallas as pl
from jax.experimental.pallas import tpu as pltpu
from jax.sharding import Mesh, PartitionSpec as P

epsilon = 1e-06
gelu_coef = 0.7978845608028654
cube_coef = 0.044715
BF = jnp.bfloat16
F32 = jnp.float32
CONTRACT_LAST = (((1,), (1,)), ((), ()))
CONTRACT_FIRST = (((0,), (0,)), ((), ()))
SLOTS = 4
CHUNKS = 4
COLS = 2


def gelu(pre_act):
    return (
        0.5
        * pre_act
        * (1.0 + jnp.tanh(gelu_coef * (pre_act + cube_coef * pre_act * pre_act * pre_act)))
    )


def gelu_slope(pre_act):
    inside = gelu_coef * (pre_act + cube_coef * pre_act * pre_act * pre_act)
    tangent = jnp.tanh(inside)
    return 0.5 * (1.0 + tangent) + 0.5 * pre_act * (1.0 - tangent * tangent) * gelu_coef * (
        1.0 + 3.0 * cube_coef * pre_act * pre_act
    )


def unit_of(residual):
    values = residual.astype(F32)
    scale_inv = lax.rsqrt(jnp.mean(values * values, axis=-1, keepdims=True) + epsilon)
    return values * scale_inv, scale_inv


def layer_copies(core, mine, other, layer, part, buf, sem, action, by_rows):
    half = layer // 2
    blocks = mine[0].shape[1]
    features = mine[0].shape[3]

    def run(pair):
        top = 0
        for ref in pair:
            rows = ref.shape[2]
            if by_rows:
                count = blocks // CHUNKS
                source = ref.at[half, pl.ds(part * count, count)]
                target = buf.at[:, pl.ds(top, rows), :]
            else:
                source = ref.at[half, :, :, pl.ds(part * (features // CHUNKS), features // CHUNKS)]
                target = buf.at[:, pl.ds(top, rows), :]
            top += rows
            copy = pltpu.make_async_copy(source, target, sem)
            copy.start() if action == "start" else copy.wait()

    if action == "wait":
        run(mine)
        return

    @pl.when(core == layer % 2)
    def _():
        run(mine)

    @pl.when(core != layer % 2)
    def _():
        run(other)


def forward_kernel(core_ref, x_ref, gain_ref, *refs):
    count = len(refs) - 6
    mine, other = refs[: count // 2], refs[count // 2 : count]
    xs_ref, ns_ref, as_ref, out_ref, wbuf, sems = refs[count:]
    core = core_ref[0]
    layers = gain_ref.shape[0]
    nx, block = ns_ref.shape[0], wbuf.shape[2]
    size = wbuf.shape[3]
    for part in range(CHUNKS):
        layer_copies(core, mine, other, 0, part, wbuf.at[part], sems.at[part], "start", False)
    out_ref[...] = x_ref[...]

    def layer_step(layer, carry):
        residual = out_ref[...]
        xs_ref[layer] = residual
        unit, _ = unit_of(residual)
        rounded = (unit * gain_ref[pl.ds(layer, 1), :]).astype(BF)
        for b in range(rounded.shape[1] // block):
            ns_ref[b % nx, layer, :, b // nx * block : (b // nx + 1) * block] = rounded[:, b * block : (b + 1) * block]
        for part in range(CHUNKS):
            cols = slice(part * size, (part + 1) * size)
            layer_copies(core, mine, other, layer, part, wbuf.at[part], sems.at[part], "wait", False)
            pre_act = jnp.dot(rounded, wbuf[part].reshape(-1, size), preferred_element_type=F32)
            as_ref[layer, :, cols] = pre_act
            out_ref[:, cols] = (residual[:, cols].astype(F32) + gelu(pre_act)).astype(BF)

            @pl.when(layer + 1 < layers)
            def _():
                layer_copies(core, mine, other, layer + 1, part, wbuf.at[part], sems.at[part], "start", False)

        return carry

    lax.fori_loop(0, layers, layer_step, 0)


def backward_kernel(core_ref, grad_ref, gain_ref, xs_ref, as_ref, *refs, first):
    count = len(refs) - COLS - 5
    mine, other = refs[: count // 2], refs[count // 2 : count]
    das = refs[count : count + COLS]
    gp_ref, out_ref, wbuf, dn_ref, sems = refs[count + COLS :]
    core = core_ref[0]
    layers = xs_ref.shape[0]
    features = wbuf.shape[3]
    size = features // CHUNKS
    wide = features // COLS
    for part in range(CHUNKS):
        layer_copies(core, mine, other, first + layers - 1, part, wbuf.at[part], sems.at[part], "start", True)
    out_ref[...] = grad_ref[...]

    def layer_step(step, carry):
        local = layers - 1 - step
        layer = first + local
        grad = out_ref[...].astype(F32)
        grad_pre = (grad * gelu_slope(as_ref[local])).astype(BF)
        for k in range(COLS):
            das[k][local] = grad_pre[:, k * wide : (k + 1) * wide]
        for part in range(CHUNKS):
            cols = slice(part * size, (part + 1) * size)
            layer_copies(core, mine, other, layer, part, wbuf.at[part], sems.at[part], "wait", True)
            dn_ref[:, cols] = lax.dot_general(
                grad_pre, wbuf[part].reshape(size, features), CONTRACT_LAST, preferred_element_type=F32
            )

            @pl.when(step + 1 < layers)
            def _():
                layer_copies(core, mine, other, layer - 1, part, wbuf.at[part], sems.at[part], "start", True)

        unit, scale_inv = unit_of(xs_ref[local])
        grad_norm = dn_ref[...]
        gp_ref[pl.ds(local, 1), :] = jnp.sum(grad_norm * unit, axis=0, keepdims=True)
        grad_unit = grad_norm * gain_ref[pl.ds(layer, 1), :]
        grad_in = scale_inv * (grad_unit - unit * jnp.mean(grad_unit * unit, axis=-1, keepdims=True))
        out_ref[...] = (grad + grad_in).astype(BF)
        return carry

    lax.fori_loop(0, layers, layer_step, 0)


def product_kernel(n_ref, *refs):
    halves = n_ref.shape[0]
    das, tail_ref, out_ref = refs[: 2 * halves], refs[2 * halves], refs[2 * halves + 1]
    per_half = out_ref.shape[0] // halves
    shard = out_ref.shape[1] - tail_ref.shape[1]
    wide = out_ref.shape[2]
    for h in range(halves):
        rows = jnp.concatenate([das[2 * h][...].reshape(-1, wide), das[2 * h + 1][...].reshape(-1, wide)])
        for b in range(per_half):
            out_ref[h * per_half + b, :shard, :] = jnp.dot(
                n_ref[h, b * shard : (b + 1) * shard, :], rows, preferred_element_type=F32
            ).astype(BF)
    out_ref[:, shard:, :] = tail_ref[...]


def head_kernel(x_ref, table_ref, target_ref, gain_ref, q_ref, f_ref, fp_ref, out_ref):
    features = x_ref.shape[1]
    logit_scale = float(features) ** (-0.5)
    unit, scale_inv = unit_of(x_ref[...])
    gain = gain_ref[...]
    rows = (unit * gain).astype(BF)
    f_ref[...] = rows
    logits = lax.dot_general(rows, table_ref[...], CONTRACT_LAST, preferred_element_type=F32) * logit_scale
    exp_logit = jnp.exp(logits)
    probability = exp_logit / jnp.sum(exp_logit, axis=-1, keepdims=True)
    vocab = lax.broadcasted_iota(jnp.int32, logits.shape, 1)
    onehot = (target_ref[...] == vocab).astype(F32)
    grad_logit = ((probability - onehot) * logit_scale).astype(BF)
    q_ref[...] = grad_logit
    grad_norm = jnp.dot(grad_logit, table_ref[...], preferred_element_type=F32)
    fp_ref[...] = jnp.sum(grad_norm * unit, axis=0, keepdims=True)
    grad_unit = grad_norm * gain
    grad_in = scale_inv * (grad_unit - unit * jnp.mean(grad_unit * unit, axis=-1, keepdims=True))
    out_ref[...] = grad_in.astype(BF)


VM = pl.BlockSpec(memory_space=pltpu.VMEM)
SM = pl.BlockSpec(memory_space=pltpu.SMEM)
HB = pl.BlockSpec(memory_space=pl.ANY)


def shape(dims, kind):
    return jax.ShapeDtypeStruct(dims, kind)


def forward_stage(core, x, gains, stores, nx):
    layers, (rows, features) = gains.shape[0], x.shape
    blocks = stores[0].shape[1]
    return pl.pallas_call(
        forward_kernel,
        in_specs=[SM, VM, VM] + [HB] * len(stores),
        out_specs=[VM] * 4,
        out_shape=[
            shape((layers, rows, features), BF),
            shape((nx, layers, rows, features // nx), BF),
            shape((layers, rows, features), F32),
            shape((rows, features), BF),
        ],
        scratch_shapes=[
            pltpu.VMEM((SLOTS, blocks, features // blocks, features // CHUNKS), BF),
            pltpu.SemaphoreType.DMA((SLOTS,)),
        ],
        name="forward_stage",
    )(core, x, gains, *stores)


def backward_stage(core, grad, gains, xs, pres, stores, first, layers):
    rows, features = grad.shape
    blocks = stores[0].shape[1]

    def part_of(kind):
        return pl.BlockSpec((layers, rows, features), lambda i: (first // layers, 0, 0), memory_space=pltpu.VMEM)

    return pl.pallas_call(
        functools.partial(backward_kernel, first=first),
        grid=(1,),
        in_specs=[SM, VM, VM, part_of(BF), part_of(F32)] + [HB] * len(stores),
        out_specs=[VM] * (COLS + 2),
        out_shape=[shape((layers, rows, features // COLS), BF)] * COLS
        + [shape((layers, features), F32), shape((rows, features), BF)],
        scratch_shapes=[
            pltpu.VMEM((SLOTS, blocks // CHUNKS, features // blocks, features), BF),
            pltpu.VMEM((rows, features), F32),
            pltpu.SemaphoreType.DMA((SLOTS,)),
        ],
        name="backward_stage",
    )(core, grad, gains, xs, pres, *stores)


def product_stage(n_rows, das, tails, chunk):
    halves, _, _ = n_rows.shape
    blocks, extra, features = tails.shape
    wide = features // COLS
    shard = n_rows.shape[1] * halves // blocks
    return pl.pallas_call(
        product_kernel,
        grid=(1,),
        in_specs=[VM] * (1 + 2 * halves)
        + [pl.BlockSpec((blocks, extra, wide), lambda i: (0, 0, chunk), memory_space=pltpu.VMEM)],
        out_specs=VM,
        out_shape=shape((blocks, shard + extra, wide), BF),
        name="product_stage",
    )(n_rows, *das, tails)


def head_stage(x, table, targets, gain):
    rows, features = x.shape
    return pl.pallas_call(
        head_kernel,
        in_specs=[VM] * 4,
        out_specs=[VM] * 4,
        out_shape=[
            shape((rows, table.shape[0]), BF),
            shape((rows, features), BF),
            shape((1, features), F32),
            shape((rows, features), BF),
        ],
        name="head_stage",
    )(x, table, targets, gain)


def turn(value, axis, steps):
    count = lax.axis_size(axis)
    return lax.ppermute(value, axis, [(i, (i + steps) % count) for i in range(count)])


def shift(value, axis, steps):
    count = lax.axis_size(axis)
    return lax.ppermute(value, axis, [(i, i + steps) for i in range(count) if 0 <= i + steps < count])


def pick(value, index, axis):
    return lax.dynamic_index_in_dim(value, index, axis, keepdims=False)


def in_order(own, partner, place):
    return jnp.where(place == 0, jnp.stack([own, partner]), jnp.stack([partner, own]))


def body(token_ids, target_ids, embedding, section_weight, section_gain, final_gain):
    ny, nzh, nc, nzl, nx = (lax.axis_size(a) for a in ("y", "zh", "c", "zl", "x"))
    iy, izh, ic, izl, ix = (lax.axis_index(a) for a in ("y", "zh", "c", "zl", "x"))
    features = embedding.shape[1]
    part_rows = embedding.shape[0]
    vocab_rows = part_rows * nzl * nx
    layers = nzh * nc
    shard = section_weight.shape[1]
    tokens = token_ids.size // layers
    core = ic.reshape(1)

    mine = lax.all_gather(section_weight[0], ("zh", "zl", "x"), axis=0)
    mine = mine.reshape(nzh, nzl * nx, shard, features)
    stores = [mine, turn(mine, "c", 1)]

    gain_pair = in_order(section_gain[0], turn(section_gain[0], "c", 1), ic)
    gains = in_order(gain_pair, turn(gain_pair, "zh", 1), izh).reshape(layers, features)

    ring = embedding[None]
    for axis, count in (("x", nx), ("zl", nzl)):
        reach = 1
        while reach < count:
            ring = jnp.concatenate([ring, turn(ring, axis, reach)])
            reach *= 2
    from_zl = (izl - jnp.arange(nzl)) % nzl
    from_x = (ix - jnp.arange(nx)) % nx
    owner = from_zl[:, None] * nx + from_x[None, :]
    row_ids = (owner[:, :, None] * part_rows + jnp.arange(part_rows)).reshape(-1)
    vocab_iota = jnp.arange(vocab_rows, dtype=jnp.int32)
    select = (vocab_iota[:, None] == row_ids[None, :]).astype(BF)
    table = jnp.dot(select, ring.reshape(vocab_rows, features), preferred_element_type=F32).astype(BF)

    share = izh * nc + ic
    token_own = pick(token_ids.reshape(layers, tokens), share, 0)
    target_own = pick(target_ids.reshape(layers, tokens), share, 0)
    onehot_in = (token_own[:, None] == vocab_iota[None, :]).astype(BF)
    x = jnp.dot(onehot_in, table, preferred_element_type=F32).astype(BF)

    saved = (
        jnp.zeros((layers, tokens, features), BF),
        jnp.zeros((nx, layers, tokens, features // nx), BF),
        jnp.zeros((layers, tokens, features), F32),
        x,
    )
    for stage in range(ny):
        x_in = x if stage == 0 else shift(saved[3], "y", 1)
        saved = lax.cond(
            iy == stage,
            lambda x_in, saved: tuple(forward_stage(core, x_in, gains, stores, nx)),
            lambda x_in, saved: saved,
            x_in,
            saved,
        )
    xs, ns, pres, x_top = saved

    q, f, final_part, grad = lax.cond(
        iy == ny - 1,
        lambda x_top: tuple(head_stage(x_top, table, target_own[:, None], final_gain[None, :])),
        lambda x_top: (
            jnp.zeros((tokens, vocab_rows), BF),
            jnp.zeros((tokens, features), BF),
            jnp.zeros((1, features), F32),
            jnp.zeros((tokens, features), BF),
        ),
        x_top,
    )

    wide = features // COLS
    pair = layers // nzh

    def backward(stage, grad_in, kept, first, count):
        return lax.cond(
            iy == stage,
            lambda grad_in, kept: tuple(backward_stage(core, grad_in, gains, xs, pres, stores, first, count)),
            lambda grad_in, kept: kept,
            grad_in,
            kept,
        )

    back = tuple(jnp.zeros((layers, tokens, wide), BF) for _ in range(COLS))
    back = back + (jnp.zeros((layers, features), F32), grad)
    left = jnp.where(iy == 0, onehot_in, q)
    for stage in range(ny - 1, 0, -1):
        grad_in = grad if stage == ny - 1 else shift(back[-1], "y", -1)
        back = backward(stage, grad_in, back, 0, layers)
        if stage == ny - 1:
            back, ns, left = lax.optimization_barrier((back, ns, left))

    n4 = ns.reshape(nx, nzh, nc, tokens, features // nx)
    n_swap = turn(pick(n4, 1 - ic, 2), "c", 1)
    n2 = jnp.stack([pick(n4, ic, 2), n_swap], axis=2)
    left2 = jnp.concatenate([left, turn(left, "c", 1)])

    def columns(to_x):
        return pick(n2, to_x, 0)

    n_parts = [columns(ix)] + [turn(columns((ix + k) % nx), "x", k) for k in (1, -1, 2)]
    n_rows = jnp.transpose(jnp.stack(n_parts, axis=2), (0, 4, 1, 2, 3)).reshape(nzh, nzl * shard, nc * nx * tokens)
    l_rows = pick(left2.reshape(nc * tokens, ny, nzh, nc, nzl, nx), ic, 3)
    l_rows = jnp.transpose(l_rows, (4, 2, 3, 1, 0)).reshape(-1, nc * tokens)

    grad_in = shift(back[-1], "y", -1)
    last, grad_low = [None] * nzh, grad_in
    for h in range(nzh - 1, -1, -1):
        kept = tuple(b[h * pair : (h + 1) * pair] for b in back[:-1]) + (grad_low,)
        last[h] = backward(0, grad_low, kept, h * pair, pair)
        grad_low = last[h][-1]

    def exchanged(da):
        near = (da, turn(da, "x", 1), turn(da, "x", -1))
        far = jnp.concatenate([turn(near[1][:1], "x", 1), turn(near[2][1:], "x", -1)])
        pieces = jnp.stack(near + (far,))
        return pick(pieces, ic, 1), turn(pick(pieces, 1 - ic, 1), "c", 1)

    das = {}
    for h in range(nzh - 1, -1, -1):
        for k in range(COLS):
            das[h, k] = exchanged(last[h][k])

    right = jnp.where(iy == 0, grad_low, f)
    gp4 = jnp.stack([last[h][COLS] for h in range(nzh)])
    misc_rows = 16

    def misc(which):
        return jnp.concatenate(
            [pick(gp4, which, 1), final_part, jnp.zeros((misc_rows - nzh - 1, features), F32)]
        ).astype(BF)

    swapped = turn(jnp.concatenate([right, misc(1 - ic)]), "c", 1)
    right2 = jnp.concatenate([right, swapped[:tokens]])
    rows_all = jnp.dot(l_rows, right2, preferred_element_type=F32).astype(BF).reshape(nx, -1, features)
    misc2 = (misc(ic).astype(F32) + swapped[tokens:].astype(F32)).astype(BF)

    def rows_for(to_x):
        return jnp.concatenate([pick(rows_all, to_x, 0), misc2])

    rows_sum = rows_for(ix).astype(F32)
    for k in (1, -1, 2):
        rows_sum = rows_sum + turn(rows_for((ix + k) % nx), "x", k).astype(F32)
    rows_sum = rows_sum.astype(BF)
    rows_z = rows_sum[: nzh * nzl * ny].reshape(nzh, nzl, ny, features)
    misc_sum = rows_sum[nzh * nzl * ny :]
    gain_rows = jnp.broadcast_to(misc_sum[:nzh].reshape(nzh, 1, 1, features), (nzh, nzl, 1, features))
    final_rows = jnp.broadcast_to(misc_sum[nzh], (nzh, nzl, 1, features))
    extra = 16
    empty = jnp.zeros((nzh, nzl, extra - ny - 2, features), BF)
    tails = jnp.concatenate([rows_z, gain_rows, final_rows, empty], axis=2).reshape(nzh * nzl, extra, features)

    z_axes = ("zh", "zl")
    nz = nzh * nzl
    iz = izh * nzl + izl

    def scattered(blocks, up_steps):
        def block(offset):
            return pick(blocks, (iz + offset) % nz, 0)

        total = block(0).astype(F32)
        for sign, count in ((1, up_steps), (-1, nz - 1 - up_steps)):
            moving = block(sign * count)
            for offset in range(count - 1, 0, -1):
                arrived = turn(moving, z_axes, sign)
                moving = (arrived.astype(F32) + block(sign * offset).astype(F32)).astype(BF)
            total = total + turn(moving, z_axes, sign).astype(F32)
        return total

    chunks = []
    for k in range(COLS):
        flat = [v for h in range(nzh) for v in das[h, k]]
        chunks.append(scattered(product_stage(n_rows, flat, tails, k), nz // 2 - k % 2))
    total = jnp.concatenate(chunks, axis=1)

    weight_grad = total[:shard]
    gain_grad = total[shard + ny : shard + ny + 1]
    rows_y = total[shard : shard + ny]
    final_plane = total[shard + ny + 1 : shard + ny + 2]

    def to_plane(which):
        return jnp.concatenate([pick(rows_y, which, 0)[None], final_plane])

    y_sum = to_plane(iy)
    for k in range(1, ny):
        y_sum = y_sum + turn(to_plane((iy + k) % ny), "y", k)
    return (weight_grad[None], gain_grad, y_sum[:1], y_sum[1])


def solution(mesh):
    names = ("y", "zh", "c", "zl", "x")
    inner = Mesh(mesh.devices.reshape(4, 2, 2, 4, 4), names)
    section = ("y", "zh", "c")
    group = ("zl", "x")
    in_specs = (
        P(None, group),
        P(None, group),
        P(group, None),
        P(section, group, None),
        P(section, None),
        P(),
    )
    out_specs = (
        P(section, group, None),
        P(section, None),
        P(section + group, None),
        P(),
    )
    return jax.shard_map(body, mesh=inner, in_specs=in_specs, out_specs=out_specs, check_vma=False)
```

```python
import functools

import jax
import jax.numpy as jnp
from jax import lax
from jax.experimental import pallas as pl
from jax.experimental.pallas import tpu as pltpu
from jax.sharding import Mesh, PartitionSpec as P

epsilon = 1e-06
gelu_coef = 0.7978845608028654
cube_coef = 0.044715
BF = jnp.bfloat16
F32 = jnp.float32
CONTRACT_LAST = (((1,), (1,)), ((), ()))
CONTRACT_FIRST = (((0,), (0,)), ((), ()))
SLOTS = 4
CHUNKS = 4
COLS = 2


def gelu(pre_act):
    return (
        0.5
        * pre_act
        * (1.0 + jnp.tanh(gelu_coef * (pre_act + cube_coef * pre_act * pre_act * pre_act)))
    )


def gelu_slope(pre_act):
    inside = gelu_coef * (pre_act + cube_coef * pre_act * pre_act * pre_act)
    tangent = jnp.tanh(inside)
    return 0.5 * (1.0 + tangent) + 0.5 * pre_act * (1.0 - tangent * tangent) * gelu_coef * (
        1.0 + 3.0 * cube_coef * pre_act * pre_act
    )


def unit_of(residual):
    values = residual.astype(F32)
    scale_inv = lax.rsqrt(jnp.mean(values * values, axis=-1, keepdims=True) + epsilon)
    return values * scale_inv, scale_inv


def start_chunk(pos, pieces, layer, part, buf, sem, by_rows):
    half = layer // 2
    count = len(pieces) // 2

    def run(refs):
        top, column, left, right, far_low, far_high = refs
        nx, cut = top.shape[1], top.shape[2]
        zs = far_low.shape[0]
        low = column.shape[1]
        ix = pos[1]
        size = column.shape[2] // CHUNKS

        def copy(ref, base, x):
            if by_rows:
                source = ref.at[base + part]
                target = buf.at[x, pl.ds(cut, low), :]
            else:
                source = ref.at[pl.ds(base, zs), :, pl.ds(part * size, size)]
                target = buf.at[:, x, pl.ds(cut, low), :]
            pltpu.make_async_copy(source, target, sem).start()

        if by_rows:
            source, target = top.at[half * zs + part], buf.at[:, pl.ds(0, cut), :]
        else:
            source = top.at[pl.ds(half * zs, zs), :, :, pl.ds(part * size, size)]
            target = buf.at[:, :, pl.ds(0, cut), :]
        pltpu.make_async_copy(source, target, sem).start()
        copy(column, half * zs, ix)
        copy(left, half * zs, lax.rem(ix + nx - 1, nx))
        copy(right, half * zs, lax.rem(ix + 1, nx))

        @pl.when(half == 0)
        def _():
            copy(far_low, 0, lax.rem(ix + 2, nx))

        @pl.when(half != 0)
        def _():
            copy(far_high, 0, lax.rem(ix + 2, nx))

    @pl.when(pos[0] == layer % 2)
    def _():
        run(pieces[:count])

    @pl.when(pos[0] != layer % 2)
    def _():
        run(pieces[count:])


def wait_chunk(buf, sem):
    pltpu.make_async_copy(buf, buf, sem).wait()


def forward_kernel(pos, x_ref, gain_ref, *refs):
    count = len(refs) - 6
    pieces = refs[:count]
    xs_ref, ns_ref, as_ref, out_ref, wbuf, sems = refs[count:]
    layers = gain_ref.shape[0]
    nx, block, size = wbuf.shape[2:]
    for part in range(CHUNKS):
        start_chunk(pos, pieces, 0, part, wbuf.at[part], sems.at[part], False)
    out_ref[...] = x_ref[...]

    def layer_step(layer, carry):
        residual = out_ref[...]
        xs_ref[layer] = residual
        unit, _ = unit_of(residual)
        rounded = (unit * gain_ref[pl.ds(layer, 1), :]).astype(BF)
        for b in range(rounded.shape[1] // block):
            ns_ref[b % nx, layer, :, b // nx * block : (b // nx + 1) * block] = rounded[:, b * block : (b + 1) * block]
        for part in range(CHUNKS):
            cols = slice(part * size, (part + 1) * size)
            wait_chunk(wbuf.at[part], sems.at[part])
            pre_act = jnp.dot(rounded, wbuf[part].reshape(-1, size), preferred_element_type=F32)
            as_ref[layer, :, cols] = pre_act
            out_ref[:, cols] = (residual[:, cols].astype(F32) + gelu(pre_act)).astype(BF)

            @pl.when(layer + 1 < layers)
            def _():
                start_chunk(pos, pieces, layer + 1, part, wbuf.at[part], sems.at[part], False)

        return carry

    lax.fori_loop(0, layers, layer_step, 0)


def backward_kernel(pos, grad_ref, gain_ref, xs_ref, as_ref, *refs, first):
    count = len(refs) - COLS - 5
    pieces = refs[:count]
    das = refs[count : count + COLS]
    gp_ref, out_ref, wbuf, dn_ref, sems = refs[count + COLS :]
    layers = xs_ref.shape[0]
    features = wbuf.shape[3]
    size = features // CHUNKS
    wide = features // COLS
    for part in range(CHUNKS):
        start_chunk(pos, pieces, first + layers - 1, part, wbuf.at[part], sems.at[part], True)
    out_ref[...] = grad_ref[...]

    def layer_step(step, carry):
        local = layers - 1 - step
        layer = first + local
        grad = out_ref[...].astype(F32)
        grad_pre = (grad * gelu_slope(as_ref[local])).astype(BF)
        for k in range(COLS):
            das[k][local] = grad_pre[:, k * wide : (k + 1) * wide]
        for part in range(CHUNKS):
            cols = slice(part * size, (part + 1) * size)
            wait_chunk(wbuf.at[part], sems.at[part])
            dn_ref[:, cols] = lax.dot_general(
                grad_pre, wbuf[part].reshape(size, features), CONTRACT_LAST, preferred_element_type=F32
            )

            @pl.when(step + 1 < layers)
            def _():
                start_chunk(pos, pieces, layer - 1, part, wbuf.at[part], sems.at[part], True)

        unit, scale_inv = unit_of(xs_ref[local])
        grad_norm = dn_ref[...]
        gp_ref[pl.ds(local, 1), :] = jnp.sum(grad_norm * unit, axis=0, keepdims=True)
        grad_unit = grad_norm * gain_ref[pl.ds(layer, 1), :]
        grad_in = scale_inv * (grad_unit - unit * jnp.mean(grad_unit * unit, axis=-1, keepdims=True))
        out_ref[...] = (grad + grad_in).astype(BF)
        return carry

    lax.fori_loop(0, layers, layer_step, 0)


def product_kernel(n_ref, *refs):
    halves = n_ref.shape[0]
    das, tail_ref, out_ref = refs[: 2 * halves], refs[2 * halves], refs[2 * halves + 1]
    per_half = out_ref.shape[0] // halves
    shard = out_ref.shape[1] - tail_ref.shape[1]
    wide = out_ref.shape[2]
    for h in range(halves):
        rows = jnp.concatenate([das[2 * h][...].reshape(-1, wide), das[2 * h + 1][...].reshape(-1, wide)])
        for b in range(per_half):
            out_ref[h * per_half + b, :shard, :] = jnp.dot(
                n_ref[h, b * shard : (b + 1) * shard, :], rows, preferred_element_type=F32
            ).astype(BF)
    out_ref[:, shard:, :] = tail_ref[...]


def head_kernel(x_ref, table_ref, target_ref, gain_ref, q_ref, f_ref, fp_ref, out_ref):
    features = x_ref.shape[1]
    logit_scale = float(features) ** (-0.5)
    unit, scale_inv = unit_of(x_ref[...])
    gain = gain_ref[...]
    rows = (unit * gain).astype(BF)
    f_ref[...] = rows
    logits = lax.dot_general(rows, table_ref[...], CONTRACT_LAST, preferred_element_type=F32) * logit_scale
    exp_logit = jnp.exp(logits)
    probability = exp_logit / jnp.sum(exp_logit, axis=-1, keepdims=True)
    vocab = lax.broadcasted_iota(jnp.int32, logits.shape, 1)
    onehot = (target_ref[...] == vocab).astype(F32)
    grad_logit = ((probability - onehot) * logit_scale).astype(BF)
    q_ref[...] = grad_logit
    grad_norm = jnp.dot(grad_logit, table_ref[...], preferred_element_type=F32)
    fp_ref[...] = jnp.sum(grad_norm * unit, axis=0, keepdims=True)
    grad_unit = grad_norm * gain
    grad_in = scale_inv * (grad_unit - unit * jnp.mean(grad_unit * unit, axis=-1, keepdims=True))
    out_ref[...] = grad_in.astype(BF)


VM = pl.BlockSpec(memory_space=pltpu.VMEM)
SM = pl.BlockSpec(memory_space=pltpu.SMEM)
HB = pl.BlockSpec(memory_space=pl.ANY)


def shape(dims, kind):
    return jax.ShapeDtypeStruct(dims, kind)


def forward_stage(core, x, gains, stores, nx):
    layers, (rows, features) = gains.shape[0], x.shape
    nz, blocks_x, _, _ = stores[0].shape
    rows_in = features // (nz // 2 * blocks_x)
    return pl.pallas_call(
        forward_kernel,
        in_specs=[SM, VM, VM] + [HB] * len(stores),
        out_specs=[VM] * 4,
        out_shape=[
            shape((layers, rows, features), BF),
            shape((nx, layers, rows, features // nx), BF),
            shape((layers, rows, features), F32),
            shape((rows, features), BF),
        ],
        scratch_shapes=[
            pltpu.VMEM((SLOTS, nz // 2, blocks_x, rows_in, features // CHUNKS), BF),
            pltpu.SemaphoreType.DMA((SLOTS,)),
        ],
        name="forward_stage",
    )(core, x, gains, *stores)


def backward_stage(core, grad, gains, xs, pres, stores, first, layers):
    rows, features = grad.shape
    nz, blocks_x, _, _ = stores[0].shape
    rows_in = features // (nz // 2 * blocks_x)

    def part_of(kind):
        return pl.BlockSpec((layers, rows, features), lambda i: (first // layers, 0, 0), memory_space=pltpu.VMEM)

    return pl.pallas_call(
        functools.partial(backward_kernel, first=first),
        grid=(1,),
        in_specs=[SM, VM, VM, part_of(BF), part_of(F32)] + [HB] * len(stores),
        out_specs=[VM] * (COLS + 2),
        out_shape=[shape((layers, rows, features // COLS), BF)] * COLS
        + [shape((layers, features), F32), shape((rows, features), BF)],
        scratch_shapes=[
            pltpu.VMEM((SLOTS, blocks_x, rows_in, features), BF),
            pltpu.VMEM((rows, features), F32),
            pltpu.SemaphoreType.DMA((SLOTS,)),
        ],
        name="backward_stage",
    )(core, grad, gains, xs, pres, *stores)


def product_stage(n_rows, das, tails, chunk):
    halves, _, _ = n_rows.shape
    blocks, extra, features = tails.shape
    wide = features // COLS
    shard = n_rows.shape[1] * halves // blocks
    return pl.pallas_call(
        product_kernel,
        grid=(1,),
        in_specs=[VM] * (1 + 2 * halves)
        + [pl.BlockSpec((blocks, extra, wide), lambda i: (0, 0, chunk), memory_space=pltpu.VMEM)],
        out_specs=VM,
        out_shape=shape((blocks, shard + extra, wide), BF),
        name="product_stage",
    )(n_rows, *das, tails)


def head_stage(x, table, targets, gain):
    rows, features = x.shape
    return pl.pallas_call(
        head_kernel,
        in_specs=[VM] * 4,
        out_specs=[VM] * 4,
        out_shape=[
            shape((rows, table.shape[0]), BF),
            shape((rows, features), BF),
            shape((1, features), F32),
            shape((rows, features), BF),
        ],
        name="head_stage",
    )(x, table, targets, gain)


def turn(value, axis, steps):
    count = lax.axis_size(axis)
    return lax.ppermute(value, axis, [(i, (i + steps) % count) for i in range(count)])


def shift(value, axis, steps):
    count = lax.axis_size(axis)
    return lax.ppermute(value, axis, [(i, i + steps) for i in range(count) if 0 <= i + steps < count])


def pick(value, index, axis):
    return lax.dynamic_index_in_dim(value, index, axis, keepdims=False)


def in_order(own, partner, place):
    return jnp.where(place == 0, jnp.stack([own, partner]), jnp.stack([partner, own]))


def ring_spread(value, axes, ups):
    count = lax.axis_size(axes)
    out = [(0, value)]
    moving = value
    for step in range(1, ups + 1):
        moving = turn(moving, axes, 1)
        out.append((step, moving))
    moving = value
    for step in range(1, count - ups):
        moving = turn(moving, axes, -1)
        out.append((-step, moving))
    return out


def gather_weights(own_rows):
    nzh, nzl, nx = (lax.axis_size(a) for a in ("zh", "zl", "x"))
    iz, ix = lax.axis_index(("zh", "zl")), lax.axis_index("x")
    nz = nzh * nzl
    rows, features = own_rows.shape
    cut = rows * 3 // 8
    a = own_rows[:cut]
    a_left, a_right = turn(a, "x", 1), turn(a, "x", -1)
    a_half = cut // 3
    a_far = jnp.concatenate([turn(a_left[:a_half], "x", 1), turn(a_right[a_half:], "x", -1)])
    line = jnp.zeros((nx, cut, features), BF)
    for steps, piece in ((0, a), (1, a_left), (-1, a_right), (2, a_far)):
        line = lax.dynamic_update_slice(line, piece[None], ((ix - steps) % nx, 0, 0))
    column = jnp.zeros((nz, rows - cut, features), BF)
    for steps, piece in ring_spread(own_rows[cut:], ("zh", "zl"), nz // 2 - 1):
        column = lax.dynamic_update_slice(column, piece[None], ((iz - steps) % nz, 0, 0))
    top = jnp.zeros((nz, nx, cut, features), BF)
    for steps, piece in ring_spread(line, ("zh", "zl"), nz // 2):
        top = lax.dynamic_update_slice(top, piece[None], ((iz - steps) % nz, 0, 0, 0))
    left, right = turn(column, "x", 1), turn(column, "x", -1)
    far_low, far_high = turn(left[: nz // 2], "x", 1), turn(right[nz // 2 :], "x", -1)
    own = [top, column, left, right, far_low, far_high]
    return own + [turn(piece, "c", 1) for piece in own]


def body(token_ids, target_ids, embedding, section_weight, section_gain, final_gain):
    ny, nzh, nc, nzl, nx = (lax.axis_size(a) for a in ("y", "zh", "c", "zl", "x"))
    iy, izh, ic, izl, ix = (lax.axis_index(a) for a in ("y", "zh", "c", "zl", "x"))
    features = embedding.shape[1]
    part_rows = embedding.shape[0]
    vocab_rows = part_rows * nzl * nx
    layers = nzh * nc
    shard = section_weight.shape[1]
    tokens = token_ids.size // layers
    core = jnp.stack([ic, ix])

    stores = gather_weights(section_weight[0])

    gain_pair = in_order(section_gain[0], turn(section_gain[0], "c", 1), ic)
    gains = in_order(gain_pair, turn(gain_pair, "zh", 1), izh).reshape(layers, features)

    ring = embedding[None]
    for axis, count in (("x", nx), ("zl", nzl)):
        reach = 1
        while reach < count:
            ring = jnp.concatenate([ring, turn(ring, axis, reach)])
            reach *= 2
    from_zl = (izl - jnp.arange(nzl)) % nzl
    from_x = (ix - jnp.arange(nx)) % nx
    owner = from_zl[:, None] * nx + from_x[None, :]
    row_ids = (owner[:, :, None] * part_rows + jnp.arange(part_rows)).reshape(-1)
    vocab_iota = jnp.arange(vocab_rows, dtype=jnp.int32)
    select = (vocab_iota[:, None] == row_ids[None, :]).astype(BF)
    table = jnp.dot(select, ring.reshape(vocab_rows, features), preferred_element_type=F32).astype(BF)

    share = izh * nc + ic
    token_own = pick(token_ids.reshape(layers, tokens), share, 0)
    target_own = pick(target_ids.reshape(layers, tokens), share, 0)
    onehot_in = (token_own[:, None] == vocab_iota[None, :]).astype(BF)
    x = jnp.dot(onehot_in, table, preferred_element_type=F32).astype(BF)

    saved = (
        jnp.zeros((layers, tokens, features), BF),
        jnp.zeros((nx, layers, tokens, features // nx), BF),
        jnp.zeros((layers, tokens, features), F32),
        x,
    )
    for stage in range(ny):
        x_in = x if stage == 0 else shift(saved[3], "y", 1)
        saved = lax.cond(
            iy == stage,
            lambda x_in, saved: tuple(forward_stage(core, x_in, gains, stores, nx)),
            lambda x_in, saved: saved,
            x_in,
            saved,
        )
    xs, ns, pres, x_top = saved

    q, f, final_part, grad = lax.cond(
        iy == ny - 1,
        lambda x_top: tuple(head_stage(x_top, table, target_own[:, None], final_gain[None, :])),
        lambda x_top: (
            jnp.zeros((tokens, vocab_rows), BF),
            jnp.zeros((tokens, features), BF),
            jnp.zeros((1, features), F32),
            jnp.zeros((tokens, features), BF),
        ),
        x_top,
    )

    wide = features // COLS
    pair = layers // nzh

    def backward(stage, grad_in, kept, first, count):
        return lax.cond(
            iy == stage,
            lambda grad_in, kept: tuple(backward_stage(core, grad_in, gains, xs, pres, stores, first, count)),
            lambda grad_in, kept: kept,
            grad_in,
            kept,
        )

    back = tuple(jnp.zeros((layers, tokens, wide), BF) for _ in range(COLS))
    back = back + (jnp.zeros((layers, features), F32), grad)
    left = jnp.where(iy == 0, onehot_in, q)
    for stage in range(ny - 1, 0, -1):
        grad_in = grad if stage == ny - 1 else shift(back[-1], "y", -1)
        back = backward(stage, grad_in, back, 0, layers)
        if stage == ny - 1:
            back, ns, left = lax.optimization_barrier((back, ns, left))

    n4 = ns.reshape(nx, nzh, nc, tokens, features // nx)
    n_swap = turn(pick(n4, 1 - ic, 2), "c", 1)
    n2 = jnp.stack([pick(n4, ic, 2), n_swap], axis=2)
    left2 = jnp.concatenate([left, turn(left, "c", 1)])

    def columns(to_x):
        return pick(n2, to_x, 0)

    n_parts = [columns(ix)] + [turn(columns((ix + k) % nx), "x", k) for k in (1, -1, 2)]
    n_rows = jnp.transpose(jnp.stack(n_parts, axis=2), (0, 4, 1, 2, 3)).reshape(nzh, nzl * shard, nc * nx * tokens)
    l_rows = pick(left2.reshape(nc * tokens, ny, nzh, nc, nzl, nx), ic, 3)
    l_rows = jnp.transpose(l_rows, (4, 2, 3, 1, 0)).reshape(-1, nc * tokens)

    grad_in = shift(back[-1], "y", -1)
    last, grad_low = [None] * nzh, grad_in
    for h in range(nzh - 1, -1, -1):
        kept = tuple(b[h * pair : (h + 1) * pair] for b in back[:-1]) + (grad_low,)
        last[h] = backward(0, grad_low, kept, h * pair, pair)
        grad_low = last[h][-1]

    def exchanged(da):
        near = (da, turn(da, "x", 1), turn(da, "x", -1))
        far = jnp.concatenate([turn(near[1][:1], "x", 1), turn(near[2][1:], "x", -1)])
        pieces = jnp.stack(near + (far,))
        return pick(pieces, ic, 1), turn(pick(pieces, 1 - ic, 1), "c", 1)

    das = {}
    for h in range(nzh - 1, -1, -1):
        for k in range(COLS):
            das[h, k] = exchanged(last[h][k])

    right = jnp.where(iy == 0, grad_low, f)
    gp4 = jnp.stack([last[h][COLS] for h in range(nzh)])
    misc_rows = 16

    def misc(which):
        return jnp.concatenate(
            [pick(gp4, which, 1), final_part, jnp.zeros((misc_rows - nzh - 1, features), F32)]
        ).astype(BF)

    swapped = turn(jnp.concatenate([right, misc(1 - ic)]), "c", 1)
    right2 = jnp.concatenate([right, swapped[:tokens]])
    rows_all = jnp.dot(l_rows, right2, preferred_element_type=F32).astype(BF).reshape(nx, -1, features)
    misc2 = (misc(ic).astype(F32) + swapped[tokens:].astype(F32)).astype(BF)

    def rows_for(to_x):
        return jnp.concatenate([pick(rows_all, to_x, 0), misc2])

    rows_sum = rows_for(ix).astype(F32)
    for k in (1, -1, 2):
        rows_sum = rows_sum + turn(rows_for((ix + k) % nx), "x", k).astype(F32)
    rows_sum = rows_sum.astype(BF)
    rows_z = rows_sum[: nzh * nzl * ny].reshape(nzh, nzl, ny, features)
    misc_sum = rows_sum[nzh * nzl * ny :]
    gain_rows = jnp.broadcast_to(misc_sum[:nzh].reshape(nzh, 1, 1, features), (nzh, nzl, 1, features))
    final_rows = jnp.broadcast_to(misc_sum[nzh], (nzh, nzl, 1, features))
    extra = 16
    empty = jnp.zeros((nzh, nzl, extra - ny - 2, features), BF)
    tails = jnp.concatenate([rows_z, gain_rows, final_rows, empty], axis=2).reshape(nzh * nzl, extra, features)

    z_axes = ("zh", "zl")
    nz = nzh * nzl
    iz = izh * nzl + izl

    def scattered(blocks, up_steps):
        def block(offset):
            return pick(blocks, (iz + offset) % nz, 0)

        total = block(0).astype(F32)
        for sign, count in ((1, up_steps), (-1, nz - 1 - up_steps)):
            moving = block(sign * count)
            for offset in range(count - 1, 0, -1):
                arrived = turn(moving, z_axes, sign)
                moving = (arrived.astype(F32) + block(sign * offset).astype(F32)).astype(BF)
            total = total + turn(moving, z_axes, sign).astype(F32)
        return total

    chunks = []
    for k in range(COLS):
        flat = [v for h in range(nzh) for v in das[h, k]]
        chunks.append(scattered(product_stage(n_rows, flat, tails, k), nz // 2 - k % 2))
    total = jnp.concatenate(chunks, axis=1)

    weight_grad = total[:shard]
    gain_grad = total[shard + ny : shard + ny + 1]
    rows_y = total[shard : shard + ny]
    final_plane = total[shard + ny + 1 : shard + ny + 2]

    def to_plane(which):
        return jnp.concatenate([pick(rows_y, which, 0)[None], final_plane])

    y_sum = to_plane(iy)
    for k in range(1, ny):
        y_sum = y_sum + turn(to_plane((iy + k) % ny), "y", k)
    return (weight_grad[None], gain_grad, y_sum[:1], y_sum[1])


def solution(mesh):
    names = ("y", "zh", "c", "zl", "x")
    inner = Mesh(mesh.devices.reshape(4, 2, 2, 4, 4), names)
    section = ("y", "zh", "c")
    group = ("zl", "x")
    in_specs = (
        P(None, group),
        P(None, group),
        P(group, None),
        P(section, group, None),
        P(section, None),
        P(),
    )
    out_specs = (
        P(section, group, None),
        P(section, None),
        P(section + group, None),
        P(),
    )
    return jax.shard_map(body, mesh=inner, in_specs=in_specs, out_specs=out_specs, check_vma=False)
```

```python
import functools

import jax
import jax.numpy as jnp
from jax import lax
from jax.experimental import pallas as pl
from jax.experimental.pallas import tpu as pltpu
from jax.sharding import Mesh, PartitionSpec as P


epsilon = 1e-06
gelu_coef = 0.7978845608028654
cube_coef = 0.044715
BF = jnp.bfloat16
F32 = jnp.float32
CONTRACT_LAST = (((1,), (1,)), ((), ()))
SLOTS = 4
CHUNKS = 4
COLS = 2


def gelu(pre_act):
    return (
        0.5
        * pre_act
        * (1.0 + jnp.tanh(gelu_coef * (pre_act + cube_coef * pre_act * pre_act * pre_act)))
    )


def gelu_slope(pre_act):
    inside = gelu_coef * (pre_act + cube_coef * pre_act * pre_act * pre_act)
    tangent = jnp.tanh(inside)
    return 0.5 * (1.0 + tangent) + 0.5 * pre_act * (1.0 - tangent * tangent) * gelu_coef * (
        1.0 + 3.0 * cube_coef * pre_act * pre_act
    )


def unit_of(residual):
    values = residual.astype(F32)
    scale_inv = lax.rsqrt(jnp.mean(values * values, axis=-1, keepdims=True) + epsilon)
    return values * scale_inv, scale_inv


def start_chunk(pos, pieces, layer, part, buf, sem, by_rows):
    half = layer // 2
    count = len(pieces) // 2

    def run(refs):
        top, column, left, right, far = refs
        nx, cut = top.shape[1], top.shape[2]
        zs = column.shape[0] // 2
        low = column.shape[1]
        ix = pos[1]
        size = column.shape[2] // CHUNKS

        def copy(ref, base, x):
            if by_rows:
                source = ref.at[base + part]
                target = buf.at[x, pl.ds(cut, low), :]
            else:
                source = ref.at[pl.ds(base, zs), :, pl.ds(part * size, size)]
                target = buf.at[:, x, pl.ds(cut, low), :]
            pltpu.make_async_copy(source, target, sem).start()

        if by_rows:
            source, target = top.at[half * zs + part], buf.at[:, pl.ds(0, cut), :]
        else:
            source = top.at[pl.ds(half * zs, zs), :, :, pl.ds(part * size, size)]
            target = buf.at[:, :, pl.ds(0, cut), :]
        pltpu.make_async_copy(source, target, sem).start()
        copy(column, half * zs, ix)
        copy(left, half * zs, lax.rem(ix + nx - 1, nx))
        copy(right, half * zs, lax.rem(ix + 1, nx))

        copy(far, half * zs, lax.rem(ix + 2, nx))

    @pl.when(pos[0] == layer % 2)
    def _():
        run(pieces[:count])

    @pl.when(pos[0] != layer % 2)
    def _():
        run(pieces[count:])


def wait_chunk(buf, sem):
    pltpu.make_async_copy(buf, buf, sem).wait()


def forward_kernel(pos, x_ref, gain_ref, *refs):
    count = len(refs) - 6
    pieces = refs[:count]
    xs_ref, ns_ref, as_ref, out_ref, wbuf, sems = refs[count:]
    layers = gain_ref.shape[0]
    nx, block, size = wbuf.shape[2:]
    for part in range(CHUNKS):
        start_chunk(pos, pieces, 0, part, wbuf.at[part], sems.at[part], False)
    out_ref[...] = x_ref[...]

    def layer_step(layer, carry):
        residual = out_ref[...]
        xs_ref[layer] = residual
        unit, _ = unit_of(residual)
        rounded = (unit * gain_ref[pl.ds(layer, 1), :]).astype(BF)
        for b in range(rounded.shape[1] // block):
            ns_ref[b % nx, layer, :, b // nx * block : (b // nx + 1) * block] = rounded[:, b * block : (b + 1) * block]
        for part in range(CHUNKS):
            cols = slice(part * size, (part + 1) * size)
            wait_chunk(wbuf.at[part], sems.at[part])
            pre_act = jnp.dot(rounded, wbuf[part].reshape(-1, size), preferred_element_type=F32)
            as_ref[layer, :, cols] = pre_act
            out_ref[:, cols] = (residual[:, cols].astype(F32) + gelu(pre_act)).astype(BF)

            @pl.when(layer + 1 < layers)
            def _():
                start_chunk(pos, pieces, layer + 1, part, wbuf.at[part], sems.at[part], False)

        return carry

    lax.fori_loop(0, layers, layer_step, 0)


def backward_kernel(pos, grad_ref, gain_ref, xs_ref, as_ref, *refs, first):
    count = len(refs) - 6
    pieces = refs[:count]
    da_ref, gp_ref, out_ref, wbuf, dn_ref, sems = refs[count:]
    layers = xs_ref.shape[0]
    features = wbuf.shape[3]
    size = features // CHUNKS
    for part in range(CHUNKS):
        start_chunk(pos, pieces, first + layers - 1, part, wbuf.at[part], sems.at[part], True)
    out_ref[...] = grad_ref[...]

    def layer_step(step, carry):
        local = layers - 1 - step
        layer = first + local
        grad = out_ref[...].astype(F32)
        grad_pre = (grad * gelu_slope(as_ref[local])).astype(BF)
        da_ref[local] = grad_pre
        for part in range(CHUNKS):
            cols = slice(part * size, (part + 1) * size)
            wait_chunk(wbuf.at[part], sems.at[part])
            dn_ref[:, cols] = lax.dot_general(
                grad_pre, wbuf[part].reshape(size, features), CONTRACT_LAST, preferred_element_type=F32
            )

            @pl.when(step + 1 < layers)
            def _():
                start_chunk(pos, pieces, layer - 1, part, wbuf.at[part], sems.at[part], True)

        unit, scale_inv = unit_of(xs_ref[local])
        grad_norm = dn_ref[...]
        gp_ref[pl.ds(local, 1), :] = jnp.sum(grad_norm * unit, axis=0, keepdims=True)
        grad_unit = grad_norm * gain_ref[pl.ds(layer, 1), :]
        grad_in = scale_inv * (grad_unit - unit * jnp.mean(grad_unit * unit, axis=-1, keepdims=True))
        out_ref[...] = (grad + grad_in).astype(BF)
        return carry

    lax.fori_loop(0, layers, layer_step, 0)


def product_kernel(n_ref, *refs):
    halves = n_ref.shape[0]
    das, tail_ref, out_ref = refs[: 2 * halves], refs[2 * halves], refs[2 * halves + 1]
    per_half = out_ref.shape[0] // halves
    shard = out_ref.shape[1] - tail_ref.shape[1]
    wide = out_ref.shape[2]
    for h in range(halves):
        rows = jnp.concatenate([das[2 * h][...].reshape(-1, wide), das[2 * h + 1][...].reshape(-1, wide)])
        for b in range(per_half):
            out_ref[h * per_half + b, :shard, :] = jnp.dot(
                n_ref[h, b * shard : (b + 1) * shard, :], rows, preferred_element_type=F32
            ).astype(BF)
    out_ref[:, shard:, :] = tail_ref[...]


def head_kernel(x_ref, table_ref, target_ref, gain_ref, q_ref, f_ref, fp_ref, out_ref):
    features = x_ref.shape[1]
    logit_scale = float(features) ** (-0.5)
    unit, scale_inv = unit_of(x_ref[...])
    gain = gain_ref[...]
    rows = (unit * gain).astype(BF)
    f_ref[...] = rows
    logits = lax.dot_general(rows, table_ref[...], CONTRACT_LAST, preferred_element_type=F32) * logit_scale
    exp_logit = jnp.exp(logits)
    probability = exp_logit / jnp.sum(exp_logit, axis=-1, keepdims=True)
    vocab = lax.broadcasted_iota(jnp.int32, logits.shape, 1)
    onehot = (target_ref[...] == vocab).astype(F32)
    grad_logit = ((probability - onehot) * logit_scale).astype(BF)
    q_ref[...] = grad_logit
    grad_norm = jnp.dot(grad_logit, table_ref[...], preferred_element_type=F32)
    fp_ref[...] = jnp.sum(grad_norm * unit, axis=0, keepdims=True)
    grad_unit = grad_norm * gain
    grad_in = scale_inv * (grad_unit - unit * jnp.mean(grad_unit * unit, axis=-1, keepdims=True))
    out_ref[...] = grad_in.astype(BF)


VM = pl.BlockSpec(memory_space=pltpu.VMEM)
SM = pl.BlockSpec(memory_space=pltpu.SMEM)
HB = pl.BlockSpec(memory_space=pl.ANY)


def shape(dims, kind):
    return jax.ShapeDtypeStruct(dims, kind)


def forward_stage(core, x, gains, stores, nx):
    layers, (rows, features) = gains.shape[0], x.shape
    nz, blocks_x, _, _ = stores[0].shape
    rows_in = features // (nz // 2 * blocks_x)
    return pl.pallas_call(
        forward_kernel,
        in_specs=[SM, VM, VM] + [HB] * len(stores),
        out_specs=[VM] * 4,
        out_shape=[
            shape((layers, rows, features), BF),
            shape((nx, layers, rows, features // nx), BF),
            shape((layers, rows, features), F32),
            shape((rows, features), BF),
        ],
        scratch_shapes=[
            pltpu.VMEM((SLOTS, nz // 2, blocks_x, rows_in, features // CHUNKS), BF),
            pltpu.SemaphoreType.DMA((SLOTS,)),
        ],
        name="forward_stage",
    )(core, x, gains, *stores)


def backward_stage(core, grad, gains, xs, pres, stores, first, layers):
    rows, features = grad.shape
    nz, blocks_x, _, _ = stores[0].shape
    rows_in = features // (nz // 2 * blocks_x)

    def part_of():
        return pl.BlockSpec((layers, rows, features), lambda i: (first // layers, 0, 0), memory_space=pltpu.VMEM)

    return pl.pallas_call(
        functools.partial(backward_kernel, first=first),
        grid=(1,),
        in_specs=[SM, VM, VM, part_of(), part_of()] + [HB] * len(stores),
        out_specs=[VM] * 3,
        out_shape=[
            shape((layers, rows, features), BF),
            shape((layers, features), F32),
            shape((rows, features), BF),
        ],
        scratch_shapes=[
            pltpu.VMEM((SLOTS, blocks_x, rows_in, features), BF),
            pltpu.VMEM((rows, features), F32),
            pltpu.SemaphoreType.DMA((SLOTS,)),
        ],
        name="backward_stage",
    )(core, grad, gains, xs, pres, *stores)


def product_stage(n_rows, das, tails, chunk):
    halves, _, _ = n_rows.shape
    blocks, extra, features = tails.shape
    wide = features // COLS
    shard = n_rows.shape[1] * halves // blocks
    return pl.pallas_call(
        product_kernel,
        grid=(1,),
        in_specs=[VM]
        + [pl.BlockSpec(das[0].shape[:2] + (wide,), lambda i: (0, 0, chunk), memory_space=pltpu.VMEM)] * (2 * halves)
        + [pl.BlockSpec((blocks, extra, wide), lambda i: (0, 0, chunk), memory_space=pltpu.VMEM)],
        out_specs=VM,
        out_shape=shape((blocks, shard + extra, wide), BF),
        name="product_stage",
    )(n_rows, *das, tails)


def head_stage(x, table, targets, gain):
    rows, features = x.shape
    return pl.pallas_call(
        head_kernel,
        in_specs=[VM] * 4,
        out_specs=[VM] * 4,
        out_shape=[
            shape((rows, table.shape[0]), BF),
            shape((rows, features), BF),
            shape((1, features), F32),
            shape((rows, features), BF),
        ],
        name="head_stage",
    )(x, table, targets, gain)


def turn(value, axis, steps):
    count = lax.axis_size(axis)
    return lax.ppermute(value, axis, [(i, (i + steps) % count) for i in range(count)])


def shift(value, axis, steps):
    count = lax.axis_size(axis)
    return lax.ppermute(value, axis, [(i, i + steps) for i in range(count) if 0 <= i + steps < count])


def pick(value, index, axis):
    return lax.dynamic_index_in_dim(value, index, axis, keepdims=False)


def in_order(own, partner, place):
    return jnp.where(place == 0, jnp.stack([own, partner]), jnp.stack([partner, own]))


def ring_spread(value, axes, ups):
    count = lax.axis_size(axes)
    out = [(0, value)]
    moving = value
    for step in range(1, ups + 1):
        moving = turn(moving, axes, 1)
        out.append((step, moving))
    moving = value
    for step in range(1, count - ups):
        moving = turn(moving, axes, -1)
        out.append((-step, moving))
    return out


def gather_weights(own_rows, small):
    nzh, nzl, nx = (lax.axis_size(a) for a in ("zh", "zl", "x"))
    iz, ix = lax.axis_index(("zh", "zl")), lax.axis_index("x")
    nz = nzh * nzl
    rows, features = own_rows.shape
    cut = rows * 3 // 8
    a = own_rows[:cut]
    a_left, a_right = turn(a, "x", 1), turn(a, "x", -1)
    a_half = cut // 3
    a_far = jnp.concatenate([turn(a_left[:a_half], "x", 1), turn(a_right[a_half:], "x", -1)])
    line = jnp.zeros((nx, cut, features), BF)
    for steps, piece in ((0, a), (1, a_left), (-1, a_right), (2, a_far)):
        line = lax.dynamic_update_slice(line, piece[None], ((ix - steps) % nx, 0, 0))
    column = jnp.zeros((nz, rows - cut, features), BF)
    for steps, piece in ring_spread(own_rows[cut:], ("zh", "zl"), nz // 2 - 1):
        column = lax.dynamic_update_slice(column, piece[None], ((iz - steps) % nz, 0, 0))
    line, column, small = lax.optimization_barrier((line, column, small))
    top = jnp.zeros((nz, nx, cut, features), BF)
    for steps, piece in ring_spread(line, ("zh", "zl"), nz // 2):
        top = lax.dynamic_update_slice(top, piece[None], ((iz - steps) % nz, 0, 0, 0))
    left, right = turn(column, "x", 1), turn(column, "x", -1)
    far = jnp.concatenate([turn(left[: nz // 2], "x", 1), turn(right[nz // 2 :], "x", -1)])
    own = [top, column, left, right, far]
    return own + [turn(piece, "c", 1) for piece in own], small


def body(token_ids, target_ids, embedding, section_weight, section_gain, final_gain):
    ny, nzh, nc, nzl, nx = (lax.axis_size(a) for a in ("y", "zh", "c", "zl", "x"))
    iy, izh, ic, izl, ix = (lax.axis_index(a) for a in ("y", "zh", "c", "zl", "x"))
    features = embedding.shape[1]
    part_rows = embedding.shape[0]
    vocab_rows = part_rows * nzl * nx
    layers = nzh * nc
    shard = section_weight.shape[1]
    tokens = token_ids.size // layers
    core = jnp.stack([ic, ix])

    gain_pair = in_order(section_gain[0], turn(section_gain[0], "c", 1), ic)
    gains = in_order(gain_pair, turn(gain_pair, "zh", 1), izh).reshape(layers, features)

    ring = embedding[None]
    for axis, count in (("x", nx), ("zl", nzl)):
        reach = 1
        while reach < count:
            ring = jnp.concatenate([ring, turn(ring, axis, reach)])
            reach *= 2
    stores, (gains, ring) = gather_weights(section_weight[0], (gains, ring))
    from_zl = (izl - jnp.arange(nzl)) % nzl
    from_x = (ix - jnp.arange(nx)) % nx
    owner = from_zl[:, None] * nx + from_x[None, :]
    row_ids = (owner[:, :, None] * part_rows + jnp.arange(part_rows)).reshape(-1)
    vocab_iota = jnp.arange(vocab_rows, dtype=jnp.int32)
    select = (vocab_iota[:, None] == row_ids[None, :]).astype(BF)
    table = jnp.dot(select, ring.reshape(vocab_rows, features), preferred_element_type=F32).astype(BF)

    share = izh * nc + ic
    token_own = pick(token_ids.reshape(layers, tokens), share, 0)
    target_own = pick(target_ids.reshape(layers, tokens), share, 0)
    onehot_in = (token_own[:, None] == vocab_iota[None, :]).astype(BF)
    x = jnp.dot(onehot_in, table, preferred_element_type=F32).astype(BF)

    saved = (
        jnp.zeros((layers, tokens, features), BF),
        jnp.zeros((nx, layers, tokens, features // nx), BF),
        jnp.zeros((layers, tokens, features), F32),
        x,
    )
    for stage in range(ny):
        x_in = x if stage == 0 else shift(saved[3], "y", 1)
        saved = lax.cond(
            iy == stage,
            lambda x_in, saved: tuple(forward_stage(core, x_in, gains, stores, nx)),
            lambda x_in, saved: saved,
            x_in,
            saved,
        )
    xs, ns, pres, x_top = saved

    q, f, final_part, grad = lax.cond(
        iy == ny - 1,
        lambda x_top: tuple(head_stage(x_top, table, target_own[:, None], final_gain[None, :])),
        lambda x_top: (
            jnp.zeros((tokens, vocab_rows), BF),
            jnp.zeros((tokens, features), BF),
            jnp.zeros((1, features), F32),
            jnp.zeros((tokens, features), BF),
        ),
        x_top,
    )

    pair = layers // nzh

    def backward(stage, grad_in, kept, first, count):
        return lax.cond(
            iy == stage,
            lambda grad_in, kept: tuple(backward_stage(core, grad_in, gains, xs, pres, stores, first, count)),
            lambda grad_in, kept: kept,
            grad_in,
            kept,
        )

    back = (jnp.zeros((layers, tokens, features), BF), jnp.zeros((layers, features), F32), grad)
    left = jnp.where(iy == 0, onehot_in, q)
    for stage in range(ny - 1, 0, -1):
        grad_in = grad if stage == ny - 1 else shift(back[-1], "y", -1)
        back = backward(stage, grad_in, back, 0, layers)
        if stage == ny - 1:
            back, ns, left = lax.optimization_barrier((back, ns, left))

    n4 = ns.reshape(nx, nzh, nc, tokens, features // nx)
    n_swap = turn(pick(n4, 1 - ic, 2), "c", 1)
    n2 = jnp.stack([pick(n4, ic, 2), n_swap], axis=2)
    left2 = jnp.concatenate([left, turn(left, "c", 1)])

    def columns(to_x):
        return pick(n2, to_x, 0)

    n_parts = [columns(ix)] + [turn(columns((ix + k) % nx), "x", k) for k in (1, -1, 2)]
    n_rows = jnp.transpose(jnp.stack(n_parts, axis=2), (0, 4, 1, 2, 3)).reshape(nzh, nzl * shard, nc * nx * tokens)
    l_rows = pick(left2.reshape(nc * tokens, ny, nzh, nc, nzl, nx), ic, 3)
    l_rows = jnp.transpose(l_rows, (4, 2, 3, 1, 0)).reshape(-1, nc * tokens)

    grad_in = shift(back[-1], "y", -1)
    grad_in, n_rows, l_rows = lax.optimization_barrier((grad_in, n_rows, l_rows))
    last, grad_low = [None] * nzh, grad_in
    for h in range(nzh - 1, -1, -1):
        kept = tuple(b[h * pair : (h + 1) * pair] for b in back[:-1]) + (grad_low,)
        last[h] = backward(0, grad_low, kept, h * pair, pair)
        grad_low = last[h][-1]

    def exchanged(da):
        near = (da, turn(da, "x", 1), turn(da, "x", -1))
        far = jnp.concatenate([turn(near[1][:1], "x", 1), turn(near[2][1:], "x", -1)])
        pieces = jnp.stack(near + (far,))
        return pick(pieces, ic, 1), turn(pick(pieces, 1 - ic, 1), "c", 1)

    das = [None] * nzh
    for h in range(nzh - 1, -1, -1):
        das[h] = exchanged(last[h][0])

    right = jnp.where(iy == 0, grad_low, f)
    gp4 = jnp.stack([last[h][1] for h in range(nzh)])
    misc_rows = 16

    def misc(which):
        return jnp.concatenate(
            [pick(gp4, which, 1), final_part, jnp.zeros((misc_rows - nzh - 1, features), F32)]
        ).astype(BF)

    swapped = turn(jnp.concatenate([right, misc(1 - ic)]), "c", 1)
    right2 = jnp.concatenate([right, swapped[:tokens]])
    rows_all = jnp.dot(l_rows, right2, preferred_element_type=F32).astype(BF).reshape(nx, -1, features)
    misc2 = (misc(ic).astype(F32) + swapped[tokens:].astype(F32)).astype(BF)

    def rows_for(to_x):
        return jnp.concatenate([pick(rows_all, to_x, 0), misc2])

    rows_sum = rows_for(ix).astype(F32)
    for k in (1, -1, 2):
        rows_sum = rows_sum + turn(rows_for((ix + k) % nx), "x", k).astype(F32)
    rows_sum = rows_sum.astype(BF)
    rows_z = rows_sum[: nzh * nzl * ny].reshape(nzh, nzl, ny, features)
    misc_sum = rows_sum[nzh * nzl * ny :]
    gain_rows = jnp.broadcast_to(misc_sum[:nzh].reshape(nzh, 1, 1, features), (nzh, nzl, 1, features))
    final_rows = jnp.broadcast_to(misc_sum[nzh], (nzh, nzl, 1, features))
    extra = 16
    empty = jnp.zeros((nzh, nzl, extra - ny - 2, features), BF)
    tails = jnp.concatenate([rows_z, gain_rows, final_rows, empty], axis=2).reshape(nzh * nzl, extra, features)

    z_axes = ("zh", "zl")
    nz = nzh * nzl
    iz = izh * nzl + izl

    def scattered(blocks, up_steps):
        def block(offset):
            return pick(blocks, (iz + offset) % nz, 0)

        total = block(0).astype(F32)
        for sign, count in ((1, up_steps), (-1, nz - 1 - up_steps)):
            moving = block(sign * count)
            for offset in range(count - 1, 0, -1):
                arrived = turn(moving, z_axes, sign)
                moving = (arrived.astype(F32) + block(sign * offset).astype(F32)).astype(BF)
            total = total + turn(moving, z_axes, sign).astype(F32)
        return total

    chunks = []
    for k in range(COLS):
        flat = [v for pieces in das for v in pieces]
        chunks.append(scattered(product_stage(n_rows, flat, tails, k), nz // 2 - k % 2))
    total = jnp.concatenate(chunks, axis=1)

    weight_grad = total[:shard]
    gain_grad = total[shard + ny : shard + ny + 1]
    rows_y = total[shard : shard + ny]
    final_plane = total[shard + ny + 1 : shard + ny + 2]

    def to_plane(which):
        return jnp.concatenate([pick(rows_y, which, 0)[None], final_plane])

    y_sum = to_plane(iy)
    for k in range(1, ny):
        y_sum = y_sum + turn(to_plane((iy + k) % ny), "y", k)
    return (weight_grad[None], gain_grad, y_sum[:1], y_sum[1])


def solution(mesh):
    names = ("y", "zh", "c", "zl", "x")
    inner = Mesh(mesh.devices.reshape(4, 2, 2, 4, 4), names)
    section = ("y", "zh", "c")
    group = ("zl", "x")
    in_specs = (
        P(None, group),
        P(None, group),
        P(group, None),
        P(section, group, None),
        P(section, None),
        P(),
    )
    out_specs = (
        P(section, group, None),
        P(section, None),
        P(section + group, None),
        P(),
    )
    return jax.shard_map(body, mesh=inner, in_specs=in_specs, out_specs=out_specs, check_vma=False)
```

```python
import functools

import jax
import jax.numpy as jnp
from jax import lax
from jax.experimental import pallas as pl
from jax.experimental.pallas import tpu as pltpu
from jax.sharding import Mesh, PartitionSpec as P


epsilon = 1e-06
gelu_coef = 0.7978845608028654
cube_coef = 0.044715
BF = jnp.bfloat16
F32 = jnp.float32
CONTRACT_LAST = (((1,), (1,)), ((), ()))
CHUNKS = 4
SLOTS = 2 * CHUNKS
COLS = 2
LANES = 128


def gelu_and_slope(pre_act):
    tangent = jnp.tanh(gelu_coef * (pre_act + cube_coef * pre_act * pre_act * pre_act))
    slope = 0.5 * (1.0 + tangent) + 0.5 * pre_act * (1.0 - tangent * tangent) * gelu_coef * (
        1.0 + 3.0 * cube_coef * pre_act * pre_act
    )
    return 0.5 * pre_act * (1.0 + tangent), slope


def unit_of(residual):
    values = residual.astype(F32)
    scale_inv = lax.rsqrt(jnp.mean(values * values, axis=-1, keepdims=True) + epsilon)
    return values * scale_inv, scale_inv


def start_layer(pos, pieces, layer, bank, wbuf, sems, by_rows):
    half = layer // 2
    count = len(pieces) // 2

    def run(refs):
        for part in range(CHUNKS):
            slot = bank * CHUNKS + part
            top = 0
            for ref in refs:
                nz, _, rows, features = ref.shape
                zs, size = nz // 2, features // CHUNKS
                if by_rows:
                    source = ref.at[half * zs + part]
                    target = wbuf.at[slot, :, pl.ds(top, rows), :]
                else:
                    source = ref.at[pl.ds(half * zs, zs), :, :, pl.ds(part * size, size)]
                    target = wbuf.at[slot, :, :, pl.ds(top, rows), :]
                top += rows
                pltpu.make_async_copy(source, target, sems.at[slot]).start()

    @pl.when(pos[0] == layer % 2)
    def _():
        run(pieces[:count])

    @pl.when(pos[0] != layer % 2)
    def _():
        run(pieces[count:])


def wait_chunk(buf, sem):
    pltpu.make_async_copy(buf, buf, sem).wait()


def forward_kernel(pos, x_ref, gain_ref, *refs):
    count = len(refs) - 7
    pieces = refs[:count]
    xs_ref, ns_ref, slope_ref, scale_ref, out_ref, wbuf, sems = refs[count:]
    layers = gain_ref.shape[0]
    nx, block, size = wbuf.shape[2:]
    start_layer(pos, pieces, 0, 0, wbuf, sems, False)
    out_ref[...] = x_ref[...]

    def layer_step(layer, carry):
        bank = lax.rem(layer, 2)

        @pl.when(layer + 1 < layers)
        def _():
            start_layer(pos, pieces, layer + 1, 1 - bank, wbuf, sems, False)

        residual = out_ref[...]
        xs_ref[layer] = residual
        unit, scale_inv = unit_of(residual)
        scale_ref[layer] = jnp.broadcast_to(scale_inv, scale_ref.shape[1:])
        rounded = (unit * gain_ref[pl.ds(layer, 1), :]).astype(BF)
        for b in range(rounded.shape[1] // block):
            ns_ref[b % nx, layer, :, b // nx * block : (b // nx + 1) * block] = rounded[:, b * block : (b + 1) * block]
        for part in range(CHUNKS):
            cols = slice(part * size, (part + 1) * size)
            slot = bank * CHUNKS + part
            wait_chunk(wbuf.at[slot], sems.at[slot])
            pre_act = jnp.dot(rounded, wbuf[slot].reshape(-1, size), preferred_element_type=F32)
            value, slope = gelu_and_slope(pre_act)
            slope_ref[layer, :, cols] = slope
            out_ref[:, cols] = (residual[:, cols].astype(F32) + value).astype(BF)
        return carry

    lax.fori_loop(0, layers, layer_step, 0)


def backward_kernel(pos, grad_ref, gain_ref, xs_ref, slope_ref, scale_ref, *refs, first):
    count = len(refs) - 6
    pieces = refs[:count]
    da_ref, gp_ref, out_ref, wbuf, dn_ref, sems = refs[count:]
    layers = xs_ref.shape[0]
    features = wbuf.shape[3]
    size = features // CHUNKS
    start_layer(pos, pieces, first + layers - 1, 0, wbuf, sems, True)
    out_ref[...] = grad_ref[...]

    def layer_step(step, carry):
        local = layers - 1 - step
        layer = first + local
        bank = lax.rem(step, 2)

        @pl.when(step + 1 < layers)
        def _():
            start_layer(pos, pieces, layer - 1, 1 - bank, wbuf, sems, True)

        grad_pre = (out_ref[...].astype(F32) * slope_ref[local]).astype(BF)
        da_ref[local] = grad_pre
        scale_inv = scale_ref[local][:, :1]
        products = jnp.zeros((grad_pre.shape[0], size), F32)
        for part in range(CHUNKS):
            cols = slice(part * size, (part + 1) * size)
            slot = bank * CHUNKS + part
            wait_chunk(wbuf.at[slot], sems.at[slot])
            grad_norm = lax.dot_general(
                grad_pre, wbuf[slot].reshape(size, features), CONTRACT_LAST, preferred_element_type=F32
            )
            grad_times = grad_norm * (xs_ref[local, :, cols].astype(F32) * scale_inv)
            gp_ref[pl.ds(local, 1), cols] = jnp.sum(grad_times, axis=0, keepdims=True)
            gain = gain_ref[pl.ds(layer, 1), cols]
            products = products + grad_times * gain
            dn_ref[:, cols] = grad_norm * gain
        mean = jnp.sum(products, axis=-1, keepdims=True) / features
        unit = xs_ref[local].astype(F32) * scale_inv
        out_ref[...] = (out_ref[...].astype(F32) + scale_inv * (dn_ref[...] - unit * mean)).astype(BF)
        return carry

    lax.fori_loop(0, layers, layer_step, 0)


def product_kernel(n_ref, *refs):
    halves = n_ref.shape[0]
    das, tail_ref, out_ref = refs[: 2 * halves], refs[2 * halves], refs[2 * halves + 1]
    per_half = out_ref.shape[0] // halves
    shard = out_ref.shape[1] - tail_ref.shape[1]
    wide = out_ref.shape[2]
    for h in range(halves):
        rows = jnp.concatenate([das[2 * h][...].reshape(-1, wide), das[2 * h + 1][...].reshape(-1, wide)])
        for b in range(per_half):
            out_ref[h * per_half + b, :shard, :] = jnp.dot(
                n_ref[h, b * shard : (b + 1) * shard, :], rows, preferred_element_type=F32
            ).astype(BF)
    out_ref[:, shard:, :] = tail_ref[...]


def head_kernel(x_ref, table_ref, target_ref, gain_ref, q_ref, f_ref, fp_ref, out_ref):
    features = x_ref.shape[1]
    logit_scale = float(features) ** (-0.5)
    unit, scale_inv = unit_of(x_ref[...])
    gain = gain_ref[...]
    rows = (unit * gain).astype(BF)
    f_ref[...] = rows
    logits = lax.dot_general(rows, table_ref[...], CONTRACT_LAST, preferred_element_type=F32) * logit_scale
    exp_logit = jnp.exp(logits)
    probability = exp_logit / jnp.sum(exp_logit, axis=-1, keepdims=True)
    vocab = lax.broadcasted_iota(jnp.int32, logits.shape, 1)
    onehot = (target_ref[...] == vocab).astype(F32)
    grad_logit = ((probability - onehot) * logit_scale).astype(BF)
    q_ref[...] = grad_logit
    grad_norm = jnp.dot(grad_logit, table_ref[...], preferred_element_type=F32)
    fp_ref[...] = jnp.sum(grad_norm * unit, axis=0, keepdims=True)
    grad_unit = grad_norm * gain
    grad_in = scale_inv * (grad_unit - unit * jnp.mean(grad_unit * unit, axis=-1, keepdims=True))
    out_ref[...] = grad_in.astype(BF)


VM = pl.BlockSpec(memory_space=pltpu.VMEM)
SM = pl.BlockSpec(memory_space=pltpu.SMEM)
HB = pl.BlockSpec(memory_space=pl.ANY)


def shape(dims, kind):
    return jax.ShapeDtypeStruct(dims, kind)


def forward_stage(core, x, gains, stores, nx):
    layers, (rows, features) = gains.shape[0], x.shape
    nz, blocks_x, _, _ = stores[0].shape
    rows_in = features // (nz // 2 * blocks_x)
    return pl.pallas_call(
        forward_kernel,
        in_specs=[SM, VM, VM] + [HB] * len(stores),
        out_specs=[VM] * 5,
        out_shape=[
            shape((layers, rows, features), BF),
            shape((nx, layers, rows, features // nx), BF),
            shape((layers, rows, features), F32),
            shape((layers, rows, LANES), F32),
            shape((rows, features), BF),
        ],
        scratch_shapes=[
            pltpu.VMEM((SLOTS, nz // 2, blocks_x, rows_in, features // CHUNKS), BF),
            pltpu.SemaphoreType.DMA((SLOTS,)),
        ],
        name="forward_stage",
    )(core, x, gains, *stores)


def backward_stage(core, grad, gains, xs, slopes, scales, stores, first, layers):
    rows, features = grad.shape
    nz, blocks_x, _, _ = stores[0].shape
    rows_in = features // (nz // 2 * blocks_x)

    def part_of(width):
        return pl.BlockSpec((layers, rows, width), lambda i: (first // layers, 0, 0), memory_space=pltpu.VMEM)

    return pl.pallas_call(
        functools.partial(backward_kernel, first=first),
        grid=(1,),
        in_specs=[SM, VM, VM, part_of(features), part_of(features), part_of(LANES)] + [HB] * len(stores),
        out_specs=[VM] * 3,
        out_shape=[
            shape((layers, rows, features), BF),
            shape((layers, features), F32),
            shape((rows, features), BF),
        ],
        scratch_shapes=[
            pltpu.VMEM((SLOTS, blocks_x, rows_in, features), BF),
            pltpu.VMEM((rows, features), F32),
            pltpu.SemaphoreType.DMA((SLOTS,)),
        ],
        name="backward_stage",
    )(core, grad, gains, xs, slopes, scales, *stores)


def product_stage(n_rows, das, tails, chunk):
    halves, _, _ = n_rows.shape
    blocks, extra, features = tails.shape
    wide = features // COLS
    shard = n_rows.shape[1] * halves // blocks
    return pl.pallas_call(
        product_kernel,
        grid=(1,),
        in_specs=[VM]
        + [pl.BlockSpec(das[0].shape[:2] + (wide,), lambda i: (0, 0, chunk), memory_space=pltpu.VMEM)] * (2 * halves)
        + [pl.BlockSpec((blocks, extra, wide), lambda i: (0, 0, chunk), memory_space=pltpu.VMEM)],
        out_specs=VM,
        out_shape=shape((blocks, shard + extra, wide), BF),
        name="product_stage",
    )(n_rows, *das, tails)


def head_stage(x, table, targets, gain):
    rows, features = x.shape
    return pl.pallas_call(
        head_kernel,
        in_specs=[VM] * 4,
        out_specs=[VM] * 4,
        out_shape=[
            shape((rows, table.shape[0]), BF),
            shape((rows, features), BF),
            shape((1, features), F32),
            shape((rows, features), BF),
        ],
        name="head_stage",
    )(x, table, targets, gain)


def turn(value, axis, steps):
    count = lax.axis_size(axis)
    return lax.ppermute(value, axis, [(i, (i + steps) % count) for i in range(count)])


def shift(value, axis, steps):
    count = lax.axis_size(axis)
    return lax.ppermute(value, axis, [(i, i + steps) for i in range(count) if 0 <= i + steps < count])


def pick(value, index, axis):
    return lax.dynamic_index_in_dim(value, index, axis, keepdims=False)


def in_order(own, partner, place):
    return jnp.where(place == 0, jnp.stack([own, partner]), jnp.stack([partner, own]))


def ring_spread(value, axes, ups):
    count = lax.axis_size(axes)
    out = [(0, value)]
    moving = value
    for step in range(1, ups + 1):
        moving = turn(moving, axes, 1)
        out.append((step, moving))
    moving = value
    for step in range(1, count - ups):
        moving = turn(moving, axes, -1)
        out.append((-step, moving))
    return out


def gather_weights(own_rows, small):
    nzh, nzl, nx = (lax.axis_size(a) for a in ("zh", "zl", "x"))
    iz, ix = lax.axis_index(("zh", "zl")), lax.axis_index("x")
    nz = nzh * nzl
    rows, features = own_rows.shape
    cut = rows // 4
    piece_rows = (rows - cut) // 2
    wide = []
    for k in range(2):
        first = cut + k * piece_rows
        gathered = lax.all_gather(own_rows[first : first + piece_rows], ("zh", "zl", "x"), axis=0)
        wide.append(gathered.reshape(nz, nx, piece_rows, features))
    a = own_rows[:cut]
    a_left, a_right = turn(a, "x", 1), turn(a, "x", -1)
    a_far = jnp.concatenate([turn(a_left[: cut // 2], "x", 1), turn(a_right[cut // 2 :], "x", -1)])
    line = jnp.zeros((nx, cut, features), BF)
    for steps, piece in ((0, a), (1, a_left), (-1, a_right), (2, a_far)):
        line = lax.dynamic_update_slice(line, piece[None], ((ix - steps) % nx, 0, 0))
    line, small = lax.optimization_barrier((line, small))
    top = jnp.zeros((nz, nx, cut, features), BF)
    for steps, piece in ring_spread(line, ("zh", "zl"), nz // 2):
        top = lax.dynamic_update_slice(top, piece[None], ((iz - steps) % nz, 0, 0, 0))
    own = [top] + wide
    return own + [turn(piece, "c", 1) for piece in own], small


def body(token_ids, target_ids, embedding, section_weight, section_gain, final_gain):
    ny, nzh, nc, nzl, nx = (lax.axis_size(a) for a in ("y", "zh", "c", "zl", "x"))
    iy, izh, ic, izl, ix = (lax.axis_index(a) for a in ("y", "zh", "c", "zl", "x"))
    features = embedding.shape[1]
    part_rows = embedding.shape[0]
    vocab_rows = part_rows * nzl * nx
    layers = nzh * nc
    shard = section_weight.shape[1]
    tokens = token_ids.size // layers
    core = jnp.stack([ic, ix])

    gain_pair = in_order(section_gain[0], turn(section_gain[0], "c", 1), ic)
    gains = in_order(gain_pair, turn(gain_pair, "zh", 1), izh).reshape(layers, features)

    ring = embedding[None]
    for axis, count in (("x", nx), ("zl", nzl)):
        reach = 1
        while reach < count:
            ring = jnp.concatenate([ring, turn(ring, axis, reach)])
            reach *= 2
    stores, (gains, ring) = gather_weights(section_weight[0], (gains, ring))
    from_zl = (izl - jnp.arange(nzl)) % nzl
    from_x = (ix - jnp.arange(nx)) % nx
    owner = from_zl[:, None] * nx + from_x[None, :]
    row_ids = (owner[:, :, None] * part_rows + jnp.arange(part_rows)).reshape(-1)
    vocab_iota = jnp.arange(vocab_rows, dtype=jnp.int32)
    select = (vocab_iota[:, None] == row_ids[None, :]).astype(BF)
    table = jnp.dot(select, ring.reshape(vocab_rows, features), preferred_element_type=F32).astype(BF)

    share = izh * nc + ic
    token_own = pick(token_ids.reshape(layers, tokens), share, 0)
    target_own = pick(target_ids.reshape(layers, tokens), share, 0)
    onehot_in = (token_own[:, None] == vocab_iota[None, :]).astype(BF)
    x = jnp.dot(onehot_in, table, preferred_element_type=F32).astype(BF)

    saved = (
        jnp.zeros((layers, tokens, features), BF),
        jnp.zeros((nx, layers, tokens, features // nx), BF),
        jnp.zeros((layers, tokens, features), F32),
        jnp.zeros((layers, tokens, LANES), F32),
        x,
    )
    for stage in range(ny):
        x_in = x if stage == 0 else shift(saved[-1], "y", 1)
        saved = lax.cond(
            iy == stage,
            lambda x_in, saved: tuple(forward_stage(core, x_in, gains, stores, nx)),
            lambda x_in, saved: saved,
            x_in,
            saved,
        )
    xs, ns, slopes, scales, x_top = saved

    q, f, final_part, grad = lax.cond(
        iy == ny - 1,
        lambda x_top: tuple(head_stage(x_top, table, target_own[:, None], final_gain[None, :])),
        lambda x_top: (
            jnp.zeros((tokens, vocab_rows), BF),
            jnp.zeros((tokens, features), BF),
            jnp.zeros((1, features), F32),
            jnp.zeros((tokens, features), BF),
        ),
        x_top,
    )

    pair = layers // nzh

    def backward(stage, grad_in, kept, first, count):
        return lax.cond(
            iy == stage,
            lambda grad_in, kept: tuple(backward_stage(core, grad_in, gains, xs, slopes, scales, stores, first, count)),
            lambda grad_in, kept: kept,
            grad_in,
            kept,
        )

    back = (jnp.zeros((layers, tokens, features), BF), jnp.zeros((layers, features), F32), grad)
    left = jnp.where(iy == 0, onehot_in, q)
    for stage in range(ny - 1, 0, -1):
        grad_in = grad if stage == ny - 1 else shift(back[-1], "y", -1)
        back = backward(stage, grad_in, back, 0, layers)
        if stage == ny - 1:
            back, ns, left = lax.optimization_barrier((back, ns, left))

    n4 = ns.reshape(nx, nzh, nc, tokens, features // nx)
    n_swap = turn(pick(n4, 1 - ic, 2), "c", 1)
    n2 = jnp.stack([pick(n4, ic, 2), n_swap], axis=2)
    left2 = jnp.concatenate([left, turn(left, "c", 1)])

    def columns(to_x):
        return pick(n2, to_x, 0)

    n_parts = [columns(ix)] + [turn(columns((ix + k) % nx), "x", k) for k in (1, -1, 2)]
    n_rows = jnp.transpose(jnp.stack(n_parts, axis=2), (0, 4, 1, 2, 3)).reshape(nzh, nzl * shard, nc * nx * tokens)
    l_rows = pick(left2.reshape(nc * tokens, ny, nzh, nc, nzl, nx), ic, 3)
    l_rows = jnp.transpose(l_rows, (4, 2, 3, 1, 0)).reshape(-1, nc * tokens)

    grad_in = shift(back[-1], "y", -1)
    grad_in, n_rows, l_rows = lax.optimization_barrier((grad_in, n_rows, l_rows))
    last, grad_low = [None] * nzh, grad_in
    for h in range(nzh - 1, -1, -1):
        kept = tuple(b[h * pair : (h + 1) * pair] for b in back[:-1]) + (grad_low,)
        last[h] = backward(0, grad_low, kept, h * pair, pair)
        grad_low = last[h][-1]

    def exchanged(da):
        near = (da, turn(da, "x", 1), turn(da, "x", -1))
        far = jnp.concatenate([turn(near[1][:1], "x", 1), turn(near[2][1:], "x", -1)])
        pieces = jnp.stack(near + (far,))
        return pick(pieces, ic, 1), turn(pick(pieces, 1 - ic, 1), "c", 1)

    das = [None] * nzh
    for h in range(nzh - 1, -1, -1):
        das[h] = exchanged(last[h][0])

    right = jnp.where(iy == 0, grad_low, f)
    gp4 = jnp.stack([last[h][1] for h in range(nzh)])
    misc_rows = 16

    def misc(which):
        return jnp.concatenate(
            [pick(gp4, which, 1), final_part, jnp.zeros((misc_rows - nzh - 1, features), F32)]
        ).astype(BF)

    swapped = turn(jnp.concatenate([right, misc(1 - ic)]), "c", 1)
    right2 = jnp.concatenate([right, swapped[:tokens]])
    rows_all = jnp.dot(l_rows, right2, preferred_element_type=F32).astype(BF).reshape(nx, -1, features)
    misc2 = (misc(ic).astype(F32) + swapped[tokens:].astype(F32)).astype(BF)

    def rows_for(to_x):
        return jnp.concatenate([pick(rows_all, to_x, 0), misc2])

    rows_sum = rows_for(ix).astype(F32)
    for k in (1, -1, 2):
        rows_sum = rows_sum + turn(rows_for((ix + k) % nx), "x", k).astype(F32)
    rows_sum = rows_sum.astype(BF)
    rows_z = rows_sum[: nzh * nzl * ny].reshape(nzh, nzl, ny, features)
    misc_sum = rows_sum[nzh * nzl * ny :]
    gain_rows = jnp.broadcast_to(misc_sum[:nzh].reshape(nzh, 1, 1, features), (nzh, nzl, 1, features))
    final_rows = jnp.broadcast_to(misc_sum[nzh], (nzh, nzl, 1, features))
    extra = 16
    empty = jnp.zeros((nzh, nzl, extra - ny - 2, features), BF)
    tails = jnp.concatenate([rows_z, gain_rows, final_rows, empty], axis=2).reshape(nzh * nzl, extra, features)

    z_axes = ("zh", "zl")
    nz = nzh * nzl
    iz = izh * nzl + izl

    def scattered(blocks, up_steps):
        def block(offset):
            return pick(blocks, (iz + offset) % nz, 0)

        total = block(0).astype(F32)
        for sign, count in ((1, up_steps), (-1, nz - 1 - up_steps)):
            moving = block(sign * count)
            for offset in range(count - 1, 0, -1):
                arrived = turn(moving, z_axes, sign)
                moving = (arrived.astype(F32) + block(sign * offset).astype(F32)).astype(BF)
            total = total + turn(moving, z_axes, sign).astype(F32)
        return total

    chunks = []
    for k in range(COLS):
        flat = [v for pieces in das for v in pieces]
        chunks.append(scattered(product_stage(n_rows, flat, tails, k), nz // 2 - k % 2))
    total = jnp.concatenate(chunks, axis=1)

    weight_grad = total[:shard]
    gain_grad = total[shard + ny : shard + ny + 1]
    rows_y = total[shard : shard + ny]
    final_plane = total[shard + ny + 1 : shard + ny + 2]

    def to_plane(which):
        return jnp.concatenate([pick(rows_y, which, 0)[None], final_plane])

    y_sum = to_plane(iy)
    for k in range(1, ny):
        y_sum = y_sum + turn(to_plane((iy + k) % ny), "y", k)
    return (weight_grad[None], gain_grad, y_sum[:1], y_sum[1])


def solution(mesh):
    names = ("y", "zh", "c", "zl", "x")
    inner = Mesh(mesh.devices.reshape(4, 2, 2, 4, 4), names)
    section = ("y", "zh", "c")
    group = ("zl", "x")
    in_specs = (
        P(None, group),
        P(None, group),
        P(group, None),
        P(section, group, None),
        P(section, None),
        P(),
    )
    out_specs = (
        P(section, group, None),
        P(section, None),
        P(section + group, None),
        P(),
    )
    return jax.shard_map(body, mesh=inner, in_specs=in_specs, out_specs=out_specs, check_vma=False)
```

```python
import functools

import jax
import jax.numpy as jnp
from jax import lax
from jax.experimental import pallas as pl
from jax.experimental.pallas import tpu as pltpu
from jax.sharding import Mesh, PartitionSpec as P


epsilon = 1e-06
gelu_coef = 0.7978845608028654
cube_coef = 0.044715
BF = jnp.bfloat16
F32 = jnp.float32
CONTRACT_LAST = (((1,), (1,)), ((), ()))
CHUNKS = 4
SLOTS = 2 * CHUNKS
COLS = 2
LANES = 128


def gelu_and_slope(pre_act):
    tangent = jnp.tanh(gelu_coef * (pre_act + cube_coef * pre_act * pre_act * pre_act))
    slope = 0.5 * (1.0 + tangent) + 0.5 * pre_act * (1.0 - tangent * tangent) * gelu_coef * (
        1.0 + 3.0 * cube_coef * pre_act * pre_act
    )
    return 0.5 * pre_act * (1.0 + tangent), slope


def unit_of(residual):
    values = residual.astype(F32)
    scale_inv = lax.rsqrt(jnp.mean(values * values, axis=-1, keepdims=True) + epsilon)
    return values * scale_inv, scale_inv


def start_layer(pos, pieces, layer, bank, wbuf, sems, by_rows):
    half = layer // 2
    count = len(pieces) // 2

    def run(refs):
        top, *by_x = refs
        nz, nx, cut, features = top.shape
        zs, size = nz // 2, features // CHUNKS
        for part in range(CHUNKS):
            slot = bank * CHUNKS + part
            cols = pl.ds(part * size, size)
            if by_rows:
                source, target = top.at[half * zs + part], wbuf.at[slot, :, pl.ds(0, cut), :]
            else:
                source, target = top.at[pl.ds(half * zs, zs), :, :, cols], wbuf.at[slot, :, :, pl.ds(0, cut), :]
            pltpu.make_async_copy(source, target, sems.at[slot]).start()
            for ref, offset in zip(by_x, (0, nx - 1, 1, 2)):
                x = lax.rem(pos[1] + offset, nx)
                rows = pl.ds(cut, ref.shape[1])
                if by_rows:
                    source, target = ref.at[half * zs + part], wbuf.at[slot, x, rows, :]
                else:
                    source, target = ref.at[pl.ds(half * zs, zs), :, cols], wbuf.at[slot, :, x, rows, :]
                pltpu.make_async_copy(source, target, sems.at[slot]).start()

    @pl.when(pos[0] == layer % 2)
    def _():
        run(pieces[:count])

    @pl.when(pos[0] != layer % 2)
    def _():
        run(pieces[count:])


def wait_chunk(buf, sem):
    pltpu.make_async_copy(buf, buf, sem).wait()


def forward_kernel(pos, x_ref, gain_ref, *refs):
    count = len(refs) - 7
    pieces = refs[:count]
    xs_ref, ns_ref, slope_ref, scale_ref, out_ref, wbuf, sems = refs[count:]
    layers = gain_ref.shape[0]
    nx, block, size = wbuf.shape[2:]
    start_layer(pos, pieces, 0, 0, wbuf, sems, False)
    out_ref[...] = x_ref[...]

    def layer_step(layer, carry):
        bank = lax.rem(layer, 2)

        @pl.when(layer + 1 < layers)
        def _():
            start_layer(pos, pieces, layer + 1, 1 - bank, wbuf, sems, False)

        residual = out_ref[...]
        xs_ref[layer] = residual
        unit, scale_inv = unit_of(residual)
        scale_ref[layer] = jnp.broadcast_to(scale_inv, scale_ref.shape[1:])
        rounded = (unit * gain_ref[pl.ds(layer, 1), :]).astype(BF)
        for b in range(rounded.shape[1] // block):
            ns_ref[b % nx, layer, :, b // nx * block : (b // nx + 1) * block] = rounded[:, b * block : (b + 1) * block]
        for part in range(CHUNKS):
            cols = slice(part * size, (part + 1) * size)
            slot = bank * CHUNKS + part
            wait_chunk(wbuf.at[slot], sems.at[slot])
            pre_act = jnp.dot(rounded, wbuf[slot].reshape(-1, size), preferred_element_type=F32)
            value, slope = gelu_and_slope(pre_act)
            slope_ref[layer, :, cols] = slope
            out_ref[:, cols] = (residual[:, cols].astype(F32) + value).astype(BF)
        return carry

    lax.fori_loop(0, layers, layer_step, 0)


def backward_kernel(pos, grad_ref, gain_ref, xs_ref, slope_ref, scale_ref, *refs, first):
    count = len(refs) - 6
    pieces = refs[:count]
    da_ref, gp_ref, out_ref, wbuf, dn_ref, sems = refs[count:]
    layers = xs_ref.shape[0]
    features = wbuf.shape[3]
    size = features // CHUNKS
    start_layer(pos, pieces, first + layers - 1, 0, wbuf, sems, True)
    out_ref[...] = grad_ref[...]

    def layer_step(step, carry):
        local = layers - 1 - step
        layer = first + local
        bank = lax.rem(step, 2)

        @pl.when(step + 1 < layers)
        def _():
            start_layer(pos, pieces, layer - 1, 1 - bank, wbuf, sems, True)

        grad_pre = (out_ref[...].astype(F32) * slope_ref[local]).astype(BF)
        da_ref[local] = grad_pre
        scale_inv = scale_ref[local][:, :1]
        products = jnp.zeros((grad_pre.shape[0], size), F32)
        for part in range(CHUNKS):
            cols = slice(part * size, (part + 1) * size)
            slot = bank * CHUNKS + part
            wait_chunk(wbuf.at[slot], sems.at[slot])
            grad_norm = lax.dot_general(
                grad_pre, wbuf[slot].reshape(size, features), CONTRACT_LAST, preferred_element_type=F32
            )
            grad_times = grad_norm * (xs_ref[local, :, cols].astype(F32) * scale_inv)
            gp_ref[pl.ds(local, 1), cols] = jnp.sum(grad_times, axis=0, keepdims=True)
            gain = gain_ref[pl.ds(layer, 1), cols]
            products = products + grad_times * gain
            dn_ref[:, cols] = grad_norm * gain
        mean = jnp.sum(products, axis=-1, keepdims=True) / features
        unit = xs_ref[local].astype(F32) * scale_inv
        out_ref[...] = (out_ref[...].astype(F32) + scale_inv * (dn_ref[...] - unit * mean)).astype(BF)
        return carry

    lax.fori_loop(0, layers, layer_step, 0)


def product_kernel(n_ref, *refs):
    halves = n_ref.shape[0]
    das, tail_ref, out_ref = refs[: 2 * halves], refs[2 * halves], refs[2 * halves + 1]
    per_half = out_ref.shape[0] // halves
    shard = out_ref.shape[1] - tail_ref.shape[1]
    wide = out_ref.shape[2]
    for h in range(halves):
        rows = jnp.concatenate([das[2 * h][...].reshape(-1, wide), das[2 * h + 1][...].reshape(-1, wide)])
        for b in range(per_half):
            out_ref[h * per_half + b, :shard, :] = jnp.dot(
                n_ref[h, b * shard : (b + 1) * shard, :], rows, preferred_element_type=F32
            ).astype(BF)
    out_ref[:, shard:, :] = tail_ref[...]


def head_kernel(x_ref, table_ref, target_ref, gain_ref, q_ref, f_ref, fp_ref, out_ref):
    features = x_ref.shape[1]
    logit_scale = float(features) ** (-0.5)
    unit, scale_inv = unit_of(x_ref[...])
    gain = gain_ref[...]
    rows = (unit * gain).astype(BF)
    f_ref[...] = rows
    logits = lax.dot_general(rows, table_ref[...], CONTRACT_LAST, preferred_element_type=F32) * logit_scale
    exp_logit = jnp.exp(logits)
    probability = exp_logit / jnp.sum(exp_logit, axis=-1, keepdims=True)
    vocab = lax.broadcasted_iota(jnp.int32, logits.shape, 1)
    onehot = (target_ref[...] == vocab).astype(F32)
    grad_logit = ((probability - onehot) * logit_scale).astype(BF)
    q_ref[...] = grad_logit
    grad_norm = jnp.dot(grad_logit, table_ref[...], preferred_element_type=F32)
    fp_ref[...] = jnp.sum(grad_norm * unit, axis=0, keepdims=True)
    grad_unit = grad_norm * gain
    grad_in = scale_inv * (grad_unit - unit * jnp.mean(grad_unit * unit, axis=-1, keepdims=True))
    out_ref[...] = grad_in.astype(BF)


VM = pl.BlockSpec(memory_space=pltpu.VMEM)
SM = pl.BlockSpec(memory_space=pltpu.SMEM)
HB = pl.BlockSpec(memory_space=pl.ANY)


def shape(dims, kind):
    return jax.ShapeDtypeStruct(dims, kind)


def forward_stage(core, x, gains, stores, nx):
    layers, (rows, features) = gains.shape[0], x.shape
    nz, blocks_x, _, _ = stores[0].shape
    rows_in = features // (nz // 2 * blocks_x)
    return pl.pallas_call(
        forward_kernel,
        in_specs=[SM, VM, VM] + [HB] * len(stores),
        out_specs=[VM] * 5,
        out_shape=[
            shape((layers, rows, features), BF),
            shape((nx, layers, rows, features // nx), BF),
            shape((layers, rows, features), F32),
            shape((layers, rows, LANES), F32),
            shape((rows, features), BF),
        ],
        scratch_shapes=[
            pltpu.VMEM((SLOTS, nz // 2, blocks_x, rows_in, features // CHUNKS), BF),
            pltpu.SemaphoreType.DMA((SLOTS,)),
        ],
        name="forward_stage",
    )(core, x, gains, *stores)


def backward_stage(core, grad, gains, xs, slopes, scales, stores, first, layers):
    rows, features = grad.shape
    nz, blocks_x, _, _ = stores[0].shape
    rows_in = features // (nz // 2 * blocks_x)

    def part_of(width):
        return pl.BlockSpec((layers, rows, width), lambda i: (first // layers, 0, 0), memory_space=pltpu.VMEM)

    return pl.pallas_call(
        functools.partial(backward_kernel, first=first),
        grid=(1,),
        in_specs=[SM, VM, VM, part_of(features), part_of(features), part_of(LANES)] + [HB] * len(stores),
        out_specs=[VM] * 3,
        out_shape=[
            shape((layers, rows, features), BF),
            shape((layers, features), F32),
            shape((rows, features), BF),
        ],
        scratch_shapes=[
            pltpu.VMEM((SLOTS, blocks_x, rows_in, features), BF),
            pltpu.VMEM((rows, features), F32),
            pltpu.SemaphoreType.DMA((SLOTS,)),
        ],
        name="backward_stage",
    )(core, grad, gains, xs, slopes, scales, *stores)


def product_stage(n_rows, das, tails, chunk):
    halves, _, _ = n_rows.shape
    blocks, extra, features = tails.shape
    wide = features // COLS
    shard = n_rows.shape[1] * halves // blocks
    return pl.pallas_call(
        product_kernel,
        grid=(1,),
        in_specs=[VM]
        + [pl.BlockSpec(das[0].shape[:2] + (wide,), lambda i: (0, 0, chunk), memory_space=pltpu.VMEM)] * (2 * halves)
        + [pl.BlockSpec((blocks, extra, wide), lambda i: (0, 0, chunk), memory_space=pltpu.VMEM)],
        out_specs=VM,
        out_shape=shape((blocks, shard + extra, wide), BF),
        name="product_stage",
    )(n_rows, *das, tails)


def head_stage(x, table, targets, gain):
    rows, features = x.shape
    return pl.pallas_call(
        head_kernel,
        in_specs=[VM] * 4,
        out_specs=[VM] * 4,
        out_shape=[
            shape((rows, table.shape[0]), BF),
            shape((rows, features), BF),
            shape((1, features), F32),
            shape((rows, features), BF),
        ],
        name="head_stage",
    )(x, table, targets, gain)


def turn(value, axis, steps):
    count = lax.axis_size(axis)
    return lax.ppermute(value, axis, [(i, (i + steps) % count) for i in range(count)])


def shift(value, axis, steps):
    count = lax.axis_size(axis)
    return lax.ppermute(value, axis, [(i, i + steps) for i in range(count) if 0 <= i + steps < count])


def pick(value, index, axis):
    return lax.dynamic_index_in_dim(value, index, axis, keepdims=False)


def in_order(own, partner, place):
    return jnp.where(place == 0, jnp.stack([own, partner]), jnp.stack([partner, own]))


def ring_spread(value, axes, ups, beside=None):
    count = lax.axis_size(axes)
    out = [(0, value)]
    moving = value
    for step in range(1, ups + 1):
        if step == ups and beside is not None:
            moving, beside = lax.optimization_barrier((moving, beside))
        moving = turn(moving, axes, 1)
        out.append((step, moving))
    moving = value
    for step in range(1, count - ups):
        moving = turn(moving, axes, -1)
        out.append((-step, moving))
    return out, beside


def gather_weights(own_rows, small, small_inputs):
    nzh, nzl, nx = (lax.axis_size(a) for a in ("zh", "zl", "x"))
    iz, ix = lax.axis_index(("zh", "zl")), lax.axis_index("x")
    nz = nzh * nzl
    rows, features = own_rows.shape
    cut = rows * 3 // 8
    a = own_rows[:cut]
    a_left, a_right = turn(a, "x", 1), turn(a, "x", -1)
    a_far = jnp.concatenate([turn(a_left[: cut // 3], "x", 1), turn(a_right[cut // 3 :], "x", -1)])
    line = jnp.zeros((nx, cut, features), BF)
    for steps, piece in ((0, a), (1, a_left), (-1, a_right), (2, a_far)):
        line = lax.dynamic_update_slice(line, piece[None], ((ix - steps) % nx, 0, 0))
    column = jnp.zeros((nz, rows - cut, features), BF)
    for steps, piece in ring_spread(own_rows[cut:], ("zh", "zl"), nz // 2 - 1)[0]:
        column = lax.dynamic_update_slice(column, piece[None], ((iz - steps) % nz, 0, 0))
    line, column, small_inputs = lax.optimization_barrier((line, column, small_inputs))
    top = jnp.zeros((nz, nx, cut, features), BF)
    spread, smalls = ring_spread(line, ("zh", "zl"), nz // 2, small(*small_inputs))
    for steps, piece in spread:
        top = lax.dynamic_update_slice(top, piece[None], ((iz - steps) % nz, 0, 0, 0))
    left, right = turn(column, "x", 1), turn(column, "x", -1)
    far = jnp.concatenate([turn(left[: nz // 2], "x", 1), turn(right[nz // 2 :], "x", -1)])
    own = [top, column, left, right, far]
    return own + [turn(piece, "c", 1) for piece in own], smalls


def body(token_ids, target_ids, embedding, section_weight, section_gain, final_gain):
    ny, nzh, nc, nzl, nx = (lax.axis_size(a) for a in ("y", "zh", "c", "zl", "x"))
    iy, izh, ic, izl, ix = (lax.axis_index(a) for a in ("y", "zh", "c", "zl", "x"))
    features = embedding.shape[1]
    part_rows = embedding.shape[0]
    vocab_rows = part_rows * nzl * nx
    layers = nzh * nc
    shard = section_weight.shape[1]
    tokens = token_ids.size // layers
    core = jnp.stack([ic, ix])

    vocab_iota = jnp.arange(vocab_rows, dtype=jnp.int32)
    share = izh * nc + ic
    token_own = pick(token_ids.reshape(layers, tokens), share, 0)
    target_own = pick(target_ids.reshape(layers, tokens), share, 0)
    onehot_in = (token_own[:, None] == vocab_iota[None, :]).astype(BF)

    def small(embedding, gain_row):
        gain_pair = in_order(gain_row, turn(gain_row, "c", 1), ic)
        gains = in_order(gain_pair, turn(gain_pair, "zh", 1), izh).reshape(layers, features)
        ring = embedding[None]
        for axis, count in (("x", nx), ("zl", nzl)):
            reach = 1
            while reach < count:
                ring = jnp.concatenate([ring, turn(ring, axis, reach)])
                reach *= 2
        from_zl = (izl - jnp.arange(nzl)) % nzl
        from_x = (ix - jnp.arange(nx)) % nx
        owner = from_zl[:, None] * nx + from_x[None, :]
        row_ids = (owner[:, :, None] * part_rows + jnp.arange(part_rows)).reshape(-1)
        select = (vocab_iota[:, None] == row_ids[None, :]).astype(BF)
        table = jnp.dot(select, ring.reshape(vocab_rows, features), preferred_element_type=F32).astype(BF)
        return gains, table, jnp.dot(onehot_in, table, preferred_element_type=F32).astype(BF)

    stores, (gains, table, x) = gather_weights(section_weight[0], small, (embedding, section_gain[0]))

    saved = (
        jnp.zeros((layers, tokens, features), BF),
        jnp.zeros((nx, layers, tokens, features // nx), BF),
        jnp.zeros((layers, tokens, features), F32),
        jnp.zeros((layers, tokens, LANES), F32),
        x,
    )
    for stage in range(ny):
        x_in = x if stage == 0 else shift(saved[-1], "y", 1)
        saved = lax.cond(
            iy == stage,
            lambda x_in, saved: tuple(forward_stage(core, x_in, gains, stores, nx)),
            lambda x_in, saved: saved,
            x_in,
            saved,
        )
    xs, ns, slopes, scales, x_top = saved

    q, f, final_part, grad = lax.cond(
        iy == ny - 1,
        lambda x_top: tuple(head_stage(x_top, table, target_own[:, None], final_gain[None, :])),
        lambda x_top: (
            jnp.zeros((tokens, vocab_rows), BF),
            jnp.zeros((tokens, features), BF),
            jnp.zeros((1, features), F32),
            jnp.zeros((tokens, features), BF),
        ),
        x_top,
    )

    pair = layers // nzh

    def backward(stage, grad_in, kept, first, count):
        return lax.cond(
            iy == stage,
            lambda grad_in, kept: tuple(backward_stage(core, grad_in, gains, xs, slopes, scales, stores, first, count)),
            lambda grad_in, kept: kept,
            grad_in,
            kept,
        )

    back = (jnp.zeros((layers, tokens, features), BF), jnp.zeros((layers, features), F32), grad)
    left = jnp.where(iy == 0, onehot_in, q)
    for stage in range(ny - 1, 0, -1):
        grad_in = grad if stage == ny - 1 else shift(back[-1], "y", -1)
        back = backward(stage, grad_in, back, 0, layers)
        if stage == ny - 1:
            back, ns, left = lax.optimization_barrier((back, ns, left))

    n4 = ns.reshape(nx, nzh, nc, tokens, features // nx)
    n_swap = turn(pick(n4, 1 - ic, 2), "c", 1)
    n2 = jnp.stack([pick(n4, ic, 2), n_swap], axis=2)
    left2 = jnp.concatenate([left, turn(left, "c", 1)])

    def columns(to_x):
        return pick(n2, to_x, 0)

    n_parts = [columns(ix)] + [turn(columns((ix + k) % nx), "x", k) for k in (1, -1, 2)]
    n_rows = jnp.transpose(jnp.stack(n_parts, axis=2), (0, 4, 1, 2, 3)).reshape(nzh, nzl * shard, nc * nx * tokens)
    l_rows = pick(left2.reshape(nc * tokens, ny, nzh, nc, nzl, nx), ic, 3)
    l_rows = jnp.transpose(l_rows, (4, 2, 3, 1, 0)).reshape(-1, nc * tokens)

    grad_in = shift(back[-1], "y", -1)
    grad_in, n_rows, l_rows = lax.optimization_barrier((grad_in, n_rows, l_rows))
    last, grad_low = [None] * nzh, grad_in
    for h in range(nzh - 1, -1, -1):
        kept = tuple(b[h * pair : (h + 1) * pair] for b in back[:-1]) + (grad_low,)
        last[h] = backward(0, grad_low, kept, h * pair, pair)
        grad_low = last[h][-1]

    def exchanged(da):
        near = (da, turn(da, "x", 1), turn(da, "x", -1))
        far = jnp.concatenate([turn(near[1][:1], "x", 1), turn(near[2][1:], "x", -1)])
        pieces = jnp.stack(near + (far,))
        return pick(pieces, ic, 1), turn(pick(pieces, 1 - ic, 1), "c", 1)

    das = [None] * nzh
    for h in range(nzh - 1, -1, -1):
        das[h] = exchanged(last[h][0])

    right = jnp.where(iy == 0, grad_low, f)
    gp4 = jnp.stack([last[h][1] for h in range(nzh)])
    misc_rows = 16

    def misc(which):
        return jnp.concatenate(
            [pick(gp4, which, 1), final_part, jnp.zeros((misc_rows - nzh - 1, features), F32)]
        ).astype(BF)

    swapped = turn(jnp.concatenate([right, misc(1 - ic)]), "c", 1)
    right2 = jnp.concatenate([right, swapped[:tokens]])
    rows_all = jnp.dot(l_rows, right2, preferred_element_type=F32).astype(BF).reshape(nx, -1, features)
    misc2 = (misc(ic).astype(F32) + swapped[tokens:].astype(F32)).astype(BF)

    def rows_for(to_x):
        return jnp.concatenate([pick(rows_all, to_x, 0), misc2])

    rows_sum = rows_for(ix).astype(F32)
    for k in (1, -1, 2):
        rows_sum = rows_sum + turn(rows_for((ix + k) % nx), "x", k).astype(F32)
    rows_sum = rows_sum.astype(BF)
    rows_z = rows_sum[: nzh * nzl * ny].reshape(nzh, nzl, ny, features)
    misc_sum = rows_sum[nzh * nzl * ny :]
    gain_rows = jnp.broadcast_to(misc_sum[:nzh].reshape(nzh, 1, 1, features), (nzh, nzl, 1, features))
    final_rows = jnp.broadcast_to(misc_sum[nzh], (nzh, nzl, 1, features))
    extra = 16
    empty = jnp.zeros((nzh, nzl, extra - ny - 2, features), BF)
    tails = jnp.concatenate([rows_z, gain_rows, final_rows, empty], axis=2).reshape(nzh * nzl, extra, features)

    z_axes = ("zh", "zl")
    nz = nzh * nzl
    iz = izh * nzl + izl

    def scattered(blocks, up_steps):
        def block(offset):
            return pick(blocks, (iz + offset) % nz, 0)

        total = block(0).astype(F32)
        for sign, count in ((1, up_steps), (-1, nz - 1 - up_steps)):
            moving = block(sign * count)
            for offset in range(count - 1, 0, -1):
                arrived = turn(moving, z_axes, sign)
                moving = (arrived.astype(F32) + block(sign * offset).astype(F32)).astype(BF)
            total = total + turn(moving, z_axes, sign).astype(F32)
        return total

    chunks = []
    for k in range(COLS):
        flat = [v for pieces in das for v in pieces]
        chunks.append(scattered(product_stage(n_rows, flat, tails, k), nz // 2 - k % 2))
    total = jnp.concatenate(chunks, axis=1)

    weight_grad = total[:shard]
    gain_grad = total[shard + ny : shard + ny + 1]
    rows_y = total[shard : shard + ny]
    final_plane = total[shard + ny + 1 : shard + ny + 2]

    def to_plane(which):
        return jnp.concatenate([pick(rows_y, which, 0)[None], final_plane])

    y_sum = to_plane(iy)
    for k in range(1, ny):
        y_sum = y_sum + turn(to_plane((iy + k) % ny), "y", k)
    return (weight_grad[None], gain_grad, y_sum[:1], y_sum[1])


def solution(mesh):
    names = ("y", "zh", "c", "zl", "x")
    inner = Mesh(mesh.devices.reshape(4, 2, 2, 4, 4), names)
    section = ("y", "zh", "c")
    group = ("zl", "x")
    in_specs = (
        P(None, group),
        P(None, group),
        P(group, None),
        P(section, group, None),
        P(section, None),
        P(),
    )
    out_specs = (
        P(section, group, None),
        P(section, None),
        P(section + group, None),
        P(),
    )
    return jax.shard_map(body, mesh=inner, in_specs=in_specs, out_specs=out_specs, check_vma=False)
```

```python
import functools

import jax
import jax.numpy as jnp
from jax import lax
from jax.experimental import pallas as pl
from jax.experimental.pallas import tpu as pltpu
from jax.sharding import Mesh, PartitionSpec as P


epsilon = 1e-06
gelu_coef = 0.7978845608028654
cube_coef = 0.044715
BF = jnp.bfloat16
F32 = jnp.float32
CONTRACT_LAST = (((1,), (1,)), ((), ()))
CHUNKS = 4
SLOTS = 2 * CHUNKS
COLS = 2
LANES = 128


def gelu_and_slope(pre_act):
    tangent = jnp.tanh(gelu_coef * (pre_act + cube_coef * pre_act * pre_act * pre_act))
    slope = 0.5 * (1.0 + tangent) + 0.5 * pre_act * (1.0 - tangent * tangent) * gelu_coef * (
        1.0 + 3.0 * cube_coef * pre_act * pre_act
    )
    return 0.5 * pre_act * (1.0 + tangent), slope


def unit_of(residual):
    values = residual.astype(F32)
    scale_inv = lax.rsqrt(jnp.mean(values * values, axis=-1, keepdims=True) + epsilon)
    return values * scale_inv, scale_inv


def start_layer(pos, pieces, layer, bank, wbuf, sems, by_rows):
    half = layer // 2
    count = len(pieces) // 2

    def run(refs):
        top, *by_x = refs
        nz, nx, cut, features = top.shape
        zs, size = nz // 2, features // CHUNKS
        for part in range(CHUNKS):
            slot = bank * CHUNKS + part
            cols = pl.ds(part * size, size)
            if by_rows:
                source, target = top.at[half * zs + part], wbuf.at[slot, :, pl.ds(0, cut), :]
            else:
                source, target = top.at[pl.ds(half * zs, zs), :, :, cols], wbuf.at[slot, :, :, pl.ds(0, cut), :]
            pltpu.make_async_copy(source, target, sems.at[slot]).start()
            for ref, offset in zip(by_x, (0, nx - 1, 1, 2)):
                x = lax.rem(pos[1] + offset, nx)
                rows = pl.ds(cut, ref.shape[1])
                if by_rows:
                    source, target = ref.at[half * zs + part], wbuf.at[slot, x, rows, :]
                else:
                    source, target = ref.at[pl.ds(half * zs, zs), :, cols], wbuf.at[slot, :, x, rows, :]
                pltpu.make_async_copy(source, target, sems.at[slot]).start()

    @pl.when(pos[0] == layer % 2)
    def _():
        run(pieces[:count])

    @pl.when(pos[0] != layer % 2)
    def _():
        run(pieces[count:])


def wait_chunk(buf, sem):
    pltpu.make_async_copy(buf, buf, sem).wait()


def forward_kernel(pos, x_ref, gain_ref, *refs):
    count = len(refs) - 7
    pieces = refs[:count]
    xs_ref, ns_ref, slope_ref, scale_ref, out_ref, wbuf, sems = refs[count:]
    layers = gain_ref.shape[0]
    nx, block, size = wbuf.shape[2:]
    start_layer(pos, pieces, 0, 0, wbuf, sems, False)
    out_ref[...] = x_ref[...]

    def layer_step(layer, carry):
        bank = lax.rem(layer, 2)

        @pl.when(layer + 1 < layers)
        def _():
            start_layer(pos, pieces, layer + 1, 1 - bank, wbuf, sems, False)

        residual = out_ref[...]
        xs_ref[layer] = residual
        unit, scale_inv = unit_of(residual)
        scale_ref[layer] = jnp.broadcast_to(scale_inv, scale_ref.shape[1:])
        rounded = (unit * gain_ref[pl.ds(layer, 1), :]).astype(BF)
        for b in range(rounded.shape[1] // block):
            ns_ref[b % nx, layer, :, b // nx * block : (b // nx + 1) * block] = rounded[:, b * block : (b + 1) * block]
        for part in range(CHUNKS):
            cols = slice(part * size, (part + 1) * size)
            slot = bank * CHUNKS + part
            wait_chunk(wbuf.at[slot], sems.at[slot])
            pre_act = jnp.dot(rounded, wbuf[slot].reshape(-1, size), preferred_element_type=F32)
            value, slope = gelu_and_slope(pre_act)
            slope_ref[layer, :, cols] = slope
            out_ref[:, cols] = (residual[:, cols].astype(F32) + value).astype(BF)
        return carry

    lax.fori_loop(0, layers, layer_step, 0)


def backward_kernel(pos, grad_ref, gain_ref, xs_ref, slope_ref, scale_ref, *refs, first):
    count = len(refs) - 6
    pieces = refs[:count]
    da_ref, gp_ref, out_ref, wbuf, dn_ref, sems = refs[count:]
    layers = xs_ref.shape[0]
    features = wbuf.shape[3]
    size = features // CHUNKS
    start_layer(pos, pieces, first + layers - 1, 0, wbuf, sems, True)
    out_ref[...] = grad_ref[...]

    def layer_step(step, carry):
        local = layers - 1 - step
        layer = first + local
        bank = lax.rem(step, 2)

        @pl.when(step + 1 < layers)
        def _():
            start_layer(pos, pieces, layer - 1, 1 - bank, wbuf, sems, True)

        grad_pre = (out_ref[...].astype(F32) * slope_ref[local]).astype(BF)
        da_ref[local] = grad_pre
        scale_inv = scale_ref[local][:, :1]
        products = jnp.zeros((grad_pre.shape[0], size), F32)
        for part in range(CHUNKS):
            cols = slice(part * size, (part + 1) * size)
            slot = bank * CHUNKS + part
            wait_chunk(wbuf.at[slot], sems.at[slot])
            grad_norm = lax.dot_general(
                grad_pre, wbuf[slot].reshape(size, features), CONTRACT_LAST, preferred_element_type=F32
            )
            grad_times = grad_norm * (xs_ref[local, :, cols].astype(F32) * scale_inv)
            gp_ref[pl.ds(local, 1), cols] = jnp.sum(grad_times, axis=0, keepdims=True)
            gain = gain_ref[pl.ds(layer, 1), cols]
            products = products + grad_times * gain
            dn_ref[:, cols] = grad_norm * gain
        mean = jnp.sum(products, axis=-1, keepdims=True) / features
        unit = xs_ref[local].astype(F32) * scale_inv
        out_ref[...] = (out_ref[...].astype(F32) + scale_inv * (dn_ref[...] - unit * mean)).astype(BF)
        return carry

    lax.fori_loop(0, layers, layer_step, 0)


def product_kernel(n_ref, *refs):
    halves = n_ref.shape[0]
    das, tail_ref, out_ref = refs[: 2 * halves], refs[2 * halves], refs[2 * halves + 1]
    per_half = out_ref.shape[0] // halves
    shard = out_ref.shape[1] - tail_ref.shape[1]
    wide = out_ref.shape[2]
    for h in range(halves):
        rows = jnp.concatenate([das[2 * h][...].reshape(-1, wide), das[2 * h + 1][...].reshape(-1, wide)])
        for b in range(per_half):
            out_ref[h * per_half + b, :shard, :] = jnp.dot(
                n_ref[h, b * shard : (b + 1) * shard, :], rows, preferred_element_type=F32
            ).astype(BF)
    out_ref[:, shard:, :] = tail_ref[...]


def head_kernel(x_ref, table_ref, target_ref, gain_ref, q_ref, f_ref, fp_ref, out_ref):
    features = x_ref.shape[1]
    logit_scale = float(features) ** (-0.5)
    unit, scale_inv = unit_of(x_ref[...])
    gain = gain_ref[...]
    rows = (unit * gain).astype(BF)
    f_ref[...] = rows
    logits = lax.dot_general(rows, table_ref[...], CONTRACT_LAST, preferred_element_type=F32) * logit_scale
    exp_logit = jnp.exp(logits)
    probability = exp_logit / jnp.sum(exp_logit, axis=-1, keepdims=True)
    vocab = lax.broadcasted_iota(jnp.int32, logits.shape, 1)
    onehot = (target_ref[...] == vocab).astype(F32)
    grad_logit = ((probability - onehot) * logit_scale).astype(BF)
    q_ref[...] = grad_logit
    grad_norm = jnp.dot(grad_logit, table_ref[...], preferred_element_type=F32)
    fp_ref[...] = jnp.sum(grad_norm * unit, axis=0, keepdims=True)
    grad_unit = grad_norm * gain
    grad_in = scale_inv * (grad_unit - unit * jnp.mean(grad_unit * unit, axis=-1, keepdims=True))
    out_ref[...] = grad_in.astype(BF)


VM = pl.BlockSpec(memory_space=pltpu.VMEM)
SM = pl.BlockSpec(memory_space=pltpu.SMEM)
HB = pl.BlockSpec(memory_space=pl.ANY)


def shape(dims, kind):
    return jax.ShapeDtypeStruct(dims, kind)


def forward_stage(core, x, gains, stores, nx):
    layers, (rows, features) = gains.shape[0], x.shape
    nz, blocks_x, _, _ = stores[0].shape
    rows_in = features // (nz // 2 * blocks_x)
    return pl.pallas_call(
        forward_kernel,
        in_specs=[SM, VM, VM] + [HB] * len(stores),
        out_specs=[VM] * 5,
        out_shape=[
            shape((layers, rows, features), BF),
            shape((nx, layers, rows, features // nx), BF),
            shape((layers, rows, features), F32),
            shape((layers, rows, LANES), F32),
            shape((rows, features), BF),
        ],
        scratch_shapes=[
            pltpu.VMEM((SLOTS, nz // 2, blocks_x, rows_in, features // CHUNKS), BF),
            pltpu.SemaphoreType.DMA((SLOTS,)),
        ],
        name="forward_stage",
    )(core, x, gains, *stores)


def backward_stage(core, grad, gains, xs, slopes, scales, stores, first, layers):
    rows, features = grad.shape
    nz, blocks_x, _, _ = stores[0].shape
    rows_in = features // (nz // 2 * blocks_x)

    def part_of(width):
        return pl.BlockSpec((layers, rows, width), lambda i: (first // layers, 0, 0), memory_space=pltpu.VMEM)

    return pl.pallas_call(
        functools.partial(backward_kernel, first=first),
        grid=(1,),
        in_specs=[SM, VM, VM, part_of(features), part_of(features), part_of(LANES)] + [HB] * len(stores),
        out_specs=[VM] * 3,
        out_shape=[
            shape((layers, rows, features), BF),
            shape((layers, features), F32),
            shape((rows, features), BF),
        ],
        scratch_shapes=[
            pltpu.VMEM((SLOTS, blocks_x, rows_in, features), BF),
            pltpu.VMEM((rows, features), F32),
            pltpu.SemaphoreType.DMA((SLOTS,)),
        ],
        name="backward_stage",
    )(core, grad, gains, xs, slopes, scales, *stores)


def product_stage(n_rows, das, tails, chunk):
    halves, _, _ = n_rows.shape
    blocks, extra, features = tails.shape
    wide = features // COLS
    shard = n_rows.shape[1] * halves // blocks
    return pl.pallas_call(
        product_kernel,
        grid=(1,),
        in_specs=[VM]
        + [pl.BlockSpec(das[0].shape[:2] + (wide,), lambda i: (0, 0, chunk), memory_space=pltpu.VMEM)] * (2 * halves)
        + [pl.BlockSpec((blocks, extra, wide), lambda i: (0, 0, chunk), memory_space=pltpu.VMEM)],
        out_specs=VM,
        out_shape=shape((blocks, shard + extra, wide), BF),
        name="product_stage",
    )(n_rows, *das, tails)


def head_stage(x, table, targets, gain):
    rows, features = x.shape
    return pl.pallas_call(
        head_kernel,
        in_specs=[VM] * 4,
        out_specs=[VM] * 4,
        out_shape=[
            shape((rows, table.shape[0]), BF),
            shape((rows, features), BF),
            shape((1, features), F32),
            shape((rows, features), BF),
        ],
        name="head_stage",
    )(x, table, targets, gain)


def turn(value, axis, steps):
    count = lax.axis_size(axis)
    return lax.ppermute(value, axis, [(i, (i + steps) % count) for i in range(count)])


def shift(value, axis, steps):
    count = lax.axis_size(axis)
    return lax.ppermute(value, axis, [(i, i + steps) for i in range(count) if 0 <= i + steps < count])


def pick(value, index, axis):
    return lax.dynamic_index_in_dim(value, index, axis, keepdims=False)


def in_order(own, partner, place):
    return jnp.where(place == 0, jnp.stack([own, partner]), jnp.stack([partner, own]))


def ring_spread(value, axes, ups, beside=None):
    count = lax.axis_size(axes)
    out = [(0, value)]
    moving = value
    for step in range(1, ups + 1):
        if step == ups and beside is not None:
            moving, beside = lax.optimization_barrier((moving, beside))
        moving = turn(moving, axes, 1)
        out.append((step, moving))
    moving = value
    for step in range(1, count - ups):
        moving = turn(moving, axes, -1)
        out.append((-step, moving))
    return out, beside


def gather_weights(own_rows, small, small_inputs):
    nzh, nzl, nx = (lax.axis_size(a) for a in ("zh", "zl", "x"))
    iz, ix = lax.axis_index(("zh", "zl")), lax.axis_index("x")
    nz = nzh * nzl
    rows, features = own_rows.shape
    cut = rows * 3 // 8
    a = own_rows[:cut]
    a_left, a_right = turn(a, "x", 1), turn(a, "x", -1)
    a_far = jnp.concatenate([turn(a_left[: cut // 3], "x", 1), turn(a_right[cut // 3 :], "x", -1)])
    line = jnp.zeros((nx, cut, features), BF)
    for steps, piece in ((0, a), (1, a_left), (-1, a_right), (2, a_far)):
        line = lax.dynamic_update_slice(line, piece[None], ((ix - steps) % nx, 0, 0))
    column = jnp.zeros((nz, rows - cut, features), BF)
    for steps, piece in ring_spread(own_rows[cut:], ("zh", "zl"), nz // 2 - 1)[0]:
        column = lax.dynamic_update_slice(column, piece[None], ((iz - steps) % nz, 0, 0))
    line, column = lax.optimization_barrier((line, column))
    top = jnp.zeros((nz, nx, cut, features), BF)
    spread, smalls = ring_spread(line, ("zh", "zl"), nz // 2, small(*small_inputs))
    for steps, piece in spread:
        top = lax.dynamic_update_slice(top, piece[None], ((iz - steps) % nz, 0, 0, 0))
    left, right = turn(column, "x", 1), turn(column, "x", -1)
    far = jnp.concatenate([turn(left[: nz // 2], "x", 1), turn(right[nz // 2 :], "x", -1)])
    own = [top, column, left, right, far]
    return own + [turn(piece, "c", 1) for piece in own], smalls


def body(token_ids, target_ids, embedding, section_weight, section_gain, final_gain):
    ny, nzh, nc, nzl, nx = (lax.axis_size(a) for a in ("y", "zh", "c", "zl", "x"))
    iy, izh, ic, izl, ix = (lax.axis_index(a) for a in ("y", "zh", "c", "zl", "x"))
    features = embedding.shape[1]
    part_rows = embedding.shape[0]
    vocab_rows = part_rows * nzl * nx
    layers = nzh * nc
    shard = section_weight.shape[1]
    tokens = token_ids.size // layers
    core = jnp.stack([ic, ix])

    vocab_iota = jnp.arange(vocab_rows, dtype=jnp.int32)
    share = izh * nc + ic
    token_own = pick(token_ids.reshape(layers, tokens), share, 0)
    target_own = pick(target_ids.reshape(layers, tokens), share, 0)
    onehot_in = (token_own[:, None] == vocab_iota[None, :]).astype(BF)

    def small(embedding, gain_row):
        gain_pair = in_order(gain_row, turn(gain_row, "c", 1), ic)
        gains = in_order(gain_pair, turn(gain_pair, "zh", 1), izh).reshape(layers, features)
        ring, step = embedding[None], 0
        for axis, count in (("x", nx), ("zl", nzl)):
            reach = 1
            while reach < count:
                step += 1
                ring = jnp.concatenate([ring, turn(ring, axis, reach)])
                reach *= 2
        from_zl = (izl - jnp.arange(nzl)) % nzl
        from_x = (ix - jnp.arange(nx)) % nx
        owner = from_zl[:, None] * nx + from_x[None, :]
        row_ids = (owner[:, :, None] * part_rows + jnp.arange(part_rows)).reshape(-1)
        select = (vocab_iota[:, None] == row_ids[None, :]).astype(BF)
        table = jnp.dot(select, ring.reshape(vocab_rows, features), preferred_element_type=F32).astype(BF)
        return gains, table, jnp.dot(onehot_in, table, preferred_element_type=F32).astype(BF)

    stores, (gains, table, x) = gather_weights(section_weight[0], small, (embedding, section_gain[0]))

    saved = (
        jnp.zeros((layers, tokens, features), BF),
        jnp.zeros((nx, layers, tokens, features // nx), BF),
        jnp.zeros((layers, tokens, features), F32),
        jnp.zeros((layers, tokens, LANES), F32),
        x,
    )
    for stage in range(ny):
        x_in = x if stage == 0 else shift(saved[-1], "y", 1)
        saved = lax.cond(
            iy == stage,
            lambda x_in, saved: tuple(forward_stage(core, x_in, gains, stores, nx)),
            lambda x_in, saved: saved,
            x_in,
            saved,
        )
    xs, ns, slopes, scales, x_top = saved

    q, f, final_part, grad = lax.cond(
        iy == ny - 1,
        lambda x_top: tuple(head_stage(x_top, table, target_own[:, None], final_gain[None, :])),
        lambda x_top: (
            jnp.zeros((tokens, vocab_rows), BF),
            jnp.zeros((tokens, features), BF),
            jnp.zeros((1, features), F32),
            jnp.zeros((tokens, features), BF),
        ),
        x_top,
    )

    pair = layers // nzh

    def backward(stage, grad_in, kept, first, count):
        return lax.cond(
            iy == stage,
            lambda grad_in, kept: tuple(backward_stage(core, grad_in, gains, xs, slopes, scales, stores, first, count)),
            lambda grad_in, kept: kept,
            grad_in,
            kept,
        )

    back = (jnp.zeros((layers, tokens, features), BF), jnp.zeros((layers, features), F32), grad)
    left = jnp.where(iy == 0, onehot_in, q)
    for stage in range(ny - 1, 0, -1):
        grad_in = grad if stage == ny - 1 else shift(back[-1], "y", -1)
        back = backward(stage, grad_in, back, 0, layers)
        if stage == ny - 1:
            back, ns, left = lax.optimization_barrier((back, ns, left))

    n4 = ns.reshape(nx, nzh, nc, tokens, features // nx)
    n_swap = turn(pick(n4, 1 - ic, 2), "c", 1)
    n2 = jnp.stack([pick(n4, ic, 2), n_swap], axis=2)
    left2 = jnp.concatenate([left, turn(left, "c", 1)])

    def columns(to_x):
        return pick(n2, to_x, 0)

    n_parts = [columns(ix)] + [turn(columns((ix + k) % nx), "x", k) for k in (1, -1, 2)]
    n_rows = jnp.transpose(jnp.stack(n_parts, axis=2), (0, 4, 1, 2, 3)).reshape(nzh, nzl * shard, nc * nx * tokens)
    l_rows = pick(left2.reshape(nc * tokens, ny, nzh, nc, nzl, nx), ic, 3)
    l_rows = jnp.transpose(l_rows, (4, 2, 3, 1, 0)).reshape(-1, nc * tokens)

    grad_in = shift(back[-1], "y", -1)
    grad_in, n_rows, l_rows = lax.optimization_barrier((grad_in, n_rows, l_rows))
    last, grad_low = [None] * nzh, grad_in
    for h in range(nzh - 1, -1, -1):
        kept = tuple(b[h * pair : (h + 1) * pair] for b in back[:-1]) + (grad_low,)
        last[h] = backward(0, grad_low, kept, h * pair, pair)
        grad_low = last[h][-1]

    def exchanged(da):
        near = (da, turn(da, "x", 1), turn(da, "x", -1))
        far = jnp.concatenate([turn(near[1][:1], "x", 1), turn(near[2][1:], "x", -1)])
        pieces = jnp.stack(near + (far,))
        return pick(pieces, ic, 1), turn(pick(pieces, 1 - ic, 1), "c", 1)

    das = [None] * nzh
    for h in range(nzh - 1, -1, -1):
        das[h] = exchanged(last[h][0])

    right = jnp.where(iy == 0, grad_low, f)
    gp4 = jnp.stack([last[h][1] for h in range(nzh)])
    misc_rows = 16

    def misc(which):
        return jnp.concatenate(
            [pick(gp4, which, 1), final_part, jnp.zeros((misc_rows - nzh - 1, features), F32)]
        ).astype(BF)

    swapped = turn(jnp.concatenate([right, misc(1 - ic)]), "c", 1)
    right2 = jnp.concatenate([right, swapped[:tokens]])
    rows_all = jnp.dot(l_rows, right2, preferred_element_type=F32).astype(BF).reshape(nx, -1, features)
    misc2 = (misc(ic).astype(F32) + swapped[tokens:].astype(F32)).astype(BF)

    def rows_for(to_x):
        return jnp.concatenate([pick(rows_all, to_x, 0), misc2])

    rows_sum = rows_for(ix).astype(F32)
    for k in (1, -1, 2):
        rows_sum = rows_sum + turn(rows_for((ix + k) % nx), "x", k).astype(F32)
    rows_sum = rows_sum.astype(BF)
    rows_z = rows_sum[: nzh * nzl * ny].reshape(nzh, nzl, ny, features)
    misc_sum = rows_sum[nzh * nzl * ny :]
    gain_rows = jnp.broadcast_to(misc_sum[:nzh].reshape(nzh, 1, 1, features), (nzh, nzl, 1, features))
    final_rows = jnp.broadcast_to(misc_sum[nzh], (nzh, nzl, 1, features))
    extra = 16
    empty = jnp.zeros((nzh, nzl, extra - ny - 2, features), BF)
    tails = jnp.concatenate([rows_z, gain_rows, final_rows, empty], axis=2).reshape(nzh * nzl, extra, features)

    z_axes = ("zh", "zl")
    nz = nzh * nzl
    iz = izh * nzl + izl

    def scattered(blocks, up_steps):
        def block(offset):
            return pick(blocks, (iz + offset) % nz, 0)

        total = block(0).astype(F32)
        for sign, count in ((1, up_steps), (-1, nz - 1 - up_steps)):
            moving = block(sign * count)
            for offset in range(count - 1, 0, -1):
                arrived = turn(moving, z_axes, sign)
                moving = (arrived.astype(F32) + block(sign * offset).astype(F32)).astype(BF)
            total = total + turn(moving, z_axes, sign).astype(F32)
        return total

    chunks = []
    for k in range(COLS):
        flat = [v for pieces in das for v in pieces]
        chunks.append(scattered(product_stage(n_rows, flat, tails, k), nz // 2 - k % 2))
    total = jnp.concatenate(chunks, axis=1)

    weight_grad = total[:shard]
    gain_grad = total[shard + ny : shard + ny + 1]
    rows_y = total[shard : shard + ny]
    final_plane = total[shard + ny + 1 : shard + ny + 2]

    def to_plane(which):
        return jnp.concatenate([pick(rows_y, which, 0)[None], final_plane])

    y_sum = to_plane(iy)
    for k in range(1, ny):
        y_sum = y_sum + turn(to_plane((iy + k) % ny), "y", k)
    return (weight_grad[None], gain_grad, y_sum[:1], y_sum[1])


def solution(mesh):
    names = ("y", "zh", "c", "zl", "x")
    inner = Mesh(mesh.devices.reshape(4, 2, 2, 4, 4), names)
    section = ("y", "zh", "c")
    group = ("zl", "x")
    in_specs = (
        P(None, group),
        P(None, group),
        P(group, None),
        P(section, group, None),
        P(section, None),
        P(),
    )
    out_specs = (
        P(section, group, None),
        P(section, None),
        P(section + group, None),
        P(),
    )
    return jax.shard_map(body, mesh=inner, in_specs=in_specs, out_specs=out_specs, check_vma=False)
```

```python
import functools

import jax
import jax.numpy as jnp
from jax import lax
from jax.experimental import pallas as pl
from jax.experimental.pallas import tpu as pltpu
from jax.sharding import Mesh, PartitionSpec as P


epsilon = 1e-06
gelu_coef = 0.7978845608028654
cube_coef = 0.044715
BF = jnp.bfloat16
F32 = jnp.float32
CONTRACT_LAST = (((1,), (1,)), ((), ()))
CHUNKS = 4
SLOTS = 2 * CHUNKS
COLS = 2
LANES = 128


def gelu_and_slope(pre_act):
    tangent = jnp.tanh(gelu_coef * (pre_act + cube_coef * pre_act * pre_act * pre_act))
    slope = 0.5 * (1.0 + tangent) + 0.5 * pre_act * (1.0 - tangent * tangent) * gelu_coef * (
        1.0 + 3.0 * cube_coef * pre_act * pre_act
    )
    return 0.5 * pre_act * (1.0 + tangent), slope


def unit_of(residual):
    values = residual.astype(F32)
    scale_inv = lax.rsqrt(jnp.mean(values * values, axis=-1, keepdims=True) + epsilon)
    return values * scale_inv, scale_inv


def start_chunks(pos, pieces, layer, parts, bank, wbuf, sems, by_rows):
    half = layer // 2
    count = len(pieces) // 2

    def run(refs):
        top, *by_x = refs
        nz, nx, cut, features = top.shape
        zs, size = nz // 2, features // CHUNKS
        for part in parts:
            slot = bank * CHUNKS + part
            cols = pl.ds(part * size, size)
            if by_rows:
                source, target = top.at[half * zs + part], wbuf.at[slot, :, pl.ds(0, cut), :]
            else:
                source, target = top.at[pl.ds(half * zs, zs), :, :, cols], wbuf.at[slot, :, :, pl.ds(0, cut), :]
            pltpu.make_async_copy(source, target, sems.at[slot]).start()
            for ref, offset in zip(by_x, (0, nx - 1, 1, 2)):
                x = lax.rem(pos[1] + offset, nx)
                rows = pl.ds(cut, ref.shape[1])
                if by_rows:
                    source, target = ref.at[half * zs + part], wbuf.at[slot, x, rows, :]
                else:
                    source, target = ref.at[pl.ds(half * zs, zs), :, cols], wbuf.at[slot, :, x, rows, :]
                pltpu.make_async_copy(source, target, sems.at[slot]).start()

    @pl.when(pos[0] == layer % 2)
    def _():
        run(pieces[:count])

    @pl.when(pos[0] != layer % 2)
    def _():
        run(pieces[count:])


def wait_chunk(buf, sem):
    pltpu.make_async_copy(buf, buf, sem).wait()


EARLY, LATE = range(CHUNKS // 2), range(CHUNKS // 2, CHUNKS)


def forward_kernel(pos, x_ref, gain_ref, *refs):
    count = len(refs) - 12
    pieces = refs[:count]
    xs_out, ns_out, slope_out, scale_out, out_ref, wbuf, sems = refs[count : count + 7]
    saves = refs[count + 7 : count + 11]
    save_sems = refs[count + 11]
    xs_ref, ns_ref, slope_ref, scale_ref = saves
    layers = gain_ref.shape[0]
    nx, block, size = wbuf.shape[2:]
    start_chunks(pos, pieces, 0, EARLY, 0, wbuf, sems, False)
    out_ref[...] = x_ref[...]

    def saved(layer, bank):
        targets = (xs_out.at[layer], ns_out.at[:, layer], slope_out.at[layer], scale_out.at[layer])
        return [
            pltpu.make_async_copy(ref.at[bank], target, save_sems.at[bank, k])
            for k, (ref, target) in enumerate(zip(saves, targets))
        ]

    def layer_step(layer, carry):
        bank = lax.rem(layer, 2)

        @pl.when(layer >= 2)
        def _():
            for copy in saved(layer - 2, bank):
                copy.wait()

        residual = out_ref[...]
        xs_ref[bank] = residual
        unit, scale_inv = unit_of(residual)
        scale_ref[bank] = jnp.broadcast_to(scale_inv, scale_ref.shape[1:])
        rounded = (unit * gain_ref[pl.ds(layer, 1), :]).astype(BF)
        for b in range(rounded.shape[1] // block):
            ns_ref[bank, b % nx, :, b // nx * block : (b // nx + 1) * block] = rounded[:, b * block : (b + 1) * block]
        for part in range(CHUNKS):
            cols = slice(part * size, (part + 1) * size)
            slot = bank * CHUNKS + part
            wait_chunk(wbuf.at[slot], sems.at[slot])
            if part == 0:
                start_chunks(pos, pieces, layer, LATE, bank, wbuf, sems, False)
            if part == CHUNKS // 2:

                @pl.when(layer + 1 < layers)
                def _():
                    start_chunks(pos, pieces, layer + 1, EARLY, 1 - bank, wbuf, sems, False)

            pre_act = jnp.dot(rounded, wbuf[slot].reshape(-1, size), preferred_element_type=F32)
            value, slope = gelu_and_slope(pre_act)
            slope_ref[bank, :, cols] = slope
            out_ref[:, cols] = (residual[:, cols].astype(F32) + value).astype(BF)
        for copy in saved(layer, bank):
            copy.start()
        return carry

    lax.fori_loop(0, layers, layer_step, 0)
    for layer in (layers - 2, layers - 1):
        for copy in saved(layer, layer % 2):
            copy.wait()


def backward_kernel(pos, grad_ref, gain_ref, xs_in, slope_in, scale_in, *refs, first):
    count = len(refs) - 10
    pieces = refs[:count]
    da_ref, gp_ref, out_ref, wbuf, dn_ref, sems, xs_ref, slope_ref, scale_ref, load_sems = refs[count:]
    layers = xs_ref.shape[0]
    features = wbuf.shape[3]
    size = features // CHUNKS

    def loads(local):
        return [
            pltpu.make_async_copy(source.at[first + local], ref.at[local], load_sems.at[k, local])
            for k, (source, ref) in enumerate(((slope_in, slope_ref), (scale_in, scale_ref), (xs_in, xs_ref)))
        ]

    start_chunks(pos, pieces, first + layers - 1, EARLY, 0, wbuf, sems, True)
    for local in range(layers - 1, -1, -1):
        for copy in loads(local):
            copy.start()
    out_ref[...] = grad_ref[...]

    def layer_step(step, carry):
        local = layers - 1 - step
        layer = first + local
        bank = lax.rem(step, 2)
        for copy in loads(local):
            copy.wait()
        grad_pre = (out_ref[...].astype(F32) * slope_ref[local]).astype(BF)
        da_ref[local] = grad_pre
        scale_inv = scale_ref[local][:, :1]
        products = jnp.zeros((grad_pre.shape[0], size), F32)
        for part in range(CHUNKS):
            cols = slice(part * size, (part + 1) * size)
            slot = bank * CHUNKS + part
            wait_chunk(wbuf.at[slot], sems.at[slot])
            if part == 0:
                start_chunks(pos, pieces, layer, LATE, bank, wbuf, sems, True)
            if part == CHUNKS // 2:

                @pl.when(step + 1 < layers)
                def _():
                    start_chunks(pos, pieces, layer - 1, EARLY, 1 - bank, wbuf, sems, True)

            grad_norm = lax.dot_general(
                grad_pre, wbuf[slot].reshape(size, features), CONTRACT_LAST, preferred_element_type=F32
            )
            grad_times = grad_norm * (xs_ref[local, :, cols].astype(F32) * scale_inv)
            gp_ref[pl.ds(local, 1), cols] = jnp.sum(grad_times, axis=0, keepdims=True)
            gain = gain_ref[pl.ds(layer, 1), cols]
            products = products + grad_times * gain
            dn_ref[:, cols] = grad_norm * gain
        mean = jnp.sum(products, axis=-1, keepdims=True) / features
        unit = xs_ref[local].astype(F32) * scale_inv
        out_ref[...] = (out_ref[...].astype(F32) + scale_inv * (dn_ref[...] - unit * mean)).astype(BF)
        return carry

    lax.fori_loop(0, layers, layer_step, 0)


def product_kernel(n_ref, *refs):
    halves = n_ref.shape[0]
    das, tail_ref, out_ref = refs[: 2 * halves], refs[2 * halves], refs[2 * halves + 1]
    per_half = out_ref.shape[0] // halves
    shard = out_ref.shape[1] - tail_ref.shape[1]
    wide = out_ref.shape[2]
    for h in range(halves):
        rows = jnp.concatenate([das[2 * h][...].reshape(-1, wide), das[2 * h + 1][...].reshape(-1, wide)])
        for b in range(per_half):
            out_ref[h * per_half + b, :shard, :] = jnp.dot(
                n_ref[h, b * shard : (b + 1) * shard, :], rows, preferred_element_type=F32
            ).astype(BF)
    out_ref[:, shard:, :] = tail_ref[...]


def head_kernel(x_ref, table_ref, target_ref, gain_ref, q_ref, f_ref, fp_ref, out_ref):
    features = x_ref.shape[1]
    logit_scale = float(features) ** (-0.5)
    unit, scale_inv = unit_of(x_ref[...])
    gain = gain_ref[...]
    rows = (unit * gain).astype(BF)
    f_ref[...] = rows
    logits = lax.dot_general(rows, table_ref[...], CONTRACT_LAST, preferred_element_type=F32) * logit_scale
    exp_logit = jnp.exp(logits)
    probability = exp_logit / jnp.sum(exp_logit, axis=-1, keepdims=True)
    vocab = lax.broadcasted_iota(jnp.int32, logits.shape, 1)
    onehot = (target_ref[...] == vocab).astype(F32)
    grad_logit = ((probability - onehot) * logit_scale).astype(BF)
    q_ref[...] = grad_logit
    grad_norm = jnp.dot(grad_logit, table_ref[...], preferred_element_type=F32)
    fp_ref[...] = jnp.sum(grad_norm * unit, axis=0, keepdims=True)
    grad_unit = grad_norm * gain
    grad_in = scale_inv * (grad_unit - unit * jnp.mean(grad_unit * unit, axis=-1, keepdims=True))
    out_ref[...] = grad_in.astype(BF)


VM = pl.BlockSpec(memory_space=pltpu.VMEM)
SM = pl.BlockSpec(memory_space=pltpu.SMEM)
HB = pl.BlockSpec(memory_space=pl.ANY)


def shape(dims, kind):
    return jax.ShapeDtypeStruct(dims, kind)


def forward_stage(core, x, gains, stores, nx):
    layers, (rows, features) = gains.shape[0], x.shape
    nz, blocks_x, _, _ = stores[0].shape
    rows_in = features // (nz // 2 * blocks_x)
    return pl.pallas_call(
        forward_kernel,
        in_specs=[SM, VM, VM] + [HB] * len(stores),
        out_specs=[HB] * 4 + [VM],
        out_shape=[
            shape((layers, rows, features), BF),
            shape((nx, layers, rows, features // nx), BF),
            shape((layers, rows, features), F32),
            shape((layers, rows, LANES), F32),
            shape((rows, features), BF),
        ],
        scratch_shapes=[
            pltpu.VMEM((SLOTS, nz // 2, blocks_x, rows_in, features // CHUNKS), BF),
            pltpu.SemaphoreType.DMA((SLOTS,)),
            pltpu.VMEM((2, rows, features), BF),
            pltpu.VMEM((2, nx, rows, features // nx), BF),
            pltpu.VMEM((2, rows, features), F32),
            pltpu.VMEM((2, rows, LANES), F32),
            pltpu.SemaphoreType.DMA((2, 4)),
        ],
        name="forward_stage",
    )(core, x, gains, *stores)


def backward_stage(core, grad, gains, xs, slopes, scales, stores, first, layers):
    rows, features = grad.shape
    nz, blocks_x, _, _ = stores[0].shape
    rows_in = features // (nz // 2 * blocks_x)

    return pl.pallas_call(
        functools.partial(backward_kernel, first=first),
        in_specs=[SM, VM, VM, HB, HB, HB] + [HB] * len(stores),
        out_specs=[VM] * 3,
        out_shape=[
            shape((layers, rows, features), BF),
            shape((layers, features), F32),
            shape((rows, features), BF),
        ],
        scratch_shapes=[
            pltpu.VMEM((SLOTS, blocks_x, rows_in, features), BF),
            pltpu.VMEM((rows, features), F32),
            pltpu.SemaphoreType.DMA((SLOTS,)),
            pltpu.VMEM((layers, rows, features), BF),
            pltpu.VMEM((layers, rows, features), F32),
            pltpu.VMEM((layers, rows, LANES), F32),
            pltpu.SemaphoreType.DMA((3, layers)),
        ],
        name="backward_stage",
    )(core, grad, gains, xs, slopes, scales, *stores)


def product_stage(n_rows, das, tails, chunk):
    halves, _, _ = n_rows.shape
    blocks, extra, features = tails.shape
    wide = features // COLS
    shard = n_rows.shape[1] * halves // blocks
    return pl.pallas_call(
        product_kernel,
        grid=(1,),
        in_specs=[VM]
        + [pl.BlockSpec(das[0].shape[:2] + (wide,), lambda i: (0, 0, chunk), memory_space=pltpu.VMEM)] * (2 * halves)
        + [pl.BlockSpec((blocks, extra, wide), lambda i: (0, 0, chunk), memory_space=pltpu.VMEM)],
        out_specs=VM,
        out_shape=shape((blocks, shard + extra, wide), BF),
        name="product_stage",
    )(n_rows, *das, tails)


def head_stage(x, table, targets, gain):
    rows, features = x.shape
    return pl.pallas_call(
        head_kernel,
        in_specs=[VM] * 4,
        out_specs=[VM] * 4,
        out_shape=[
            shape((rows, table.shape[0]), BF),
            shape((rows, features), BF),
            shape((1, features), F32),
            shape((rows, features), BF),
        ],
        name="head_stage",
    )(x, table, targets, gain)


def turn(value, axis, steps):
    count = lax.axis_size(axis)
    return lax.ppermute(value, axis, [(i, (i + steps) % count) for i in range(count)])


def shift(value, axis, steps):
    count = lax.axis_size(axis)
    return lax.ppermute(value, axis, [(i, i + steps) for i in range(count) if 0 <= i + steps < count])


def pick(value, index, axis):
    return lax.dynamic_index_in_dim(value, index, axis, keepdims=False)


def in_order(own, partner, place):
    return jnp.where(place == 0, jnp.stack([own, partner]), jnp.stack([partner, own]))


def ring_spread(value, axes, ups, beside=None):
    count = lax.axis_size(axes)
    out = [(0, value)]
    moving = value
    for step in range(1, ups + 1):
        if step == ups and beside is not None:
            moving, beside = lax.optimization_barrier((moving, beside))
        moving = turn(moving, axes, 1)
        out.append((step, moving))
    moving = value
    for step in range(1, count - ups):
        moving = turn(moving, axes, -1)
        out.append((-step, moving))
    return out, beside


def gather_weights(own_rows, small, small_inputs):
    nzh, nzl, nx = (lax.axis_size(a) for a in ("zh", "zl", "x"))
    iz, ix = lax.axis_index(("zh", "zl")), lax.axis_index("x")
    nz = nzh * nzl
    rows, features = own_rows.shape
    cut = rows * 3 // 8
    a = own_rows[:cut]
    a_left, a_right = turn(a, "x", 1), turn(a, "x", -1)
    a_far = jnp.concatenate([turn(a_left[: cut // 3], "x", 1), turn(a_right[cut // 3 :], "x", -1)])
    line = jnp.zeros((nx, cut, features), BF)
    for steps, piece in ((0, a), (1, a_left), (-1, a_right), (2, a_far)):
        line = lax.dynamic_update_slice(line, piece[None], ((ix - steps) % nx, 0, 0))
    column = jnp.zeros((nz, rows - cut, features), BF)
    for steps, piece in ring_spread(own_rows[cut:], ("zh", "zl"), nz // 2 - 1)[0]:
        column = lax.dynamic_update_slice(column, piece[None], ((iz - steps) % nz, 0, 0))
    line, column = lax.optimization_barrier((line, column))
    top = jnp.zeros((nz, nx, cut, features), BF)
    left, right = turn(column, "x", 1), turn(column, "x", -1)
    spread, (left, right, smalls) = ring_spread(line, ("zh", "zl"), nz // 2, (left, right, small(*small_inputs)))
    for steps, piece in spread:
        top = lax.dynamic_update_slice(top, piece[None], ((iz - steps) % nz, 0, 0, 0))
    far = jnp.concatenate([turn(left[: nz // 2], "x", 1), turn(right[nz // 2 :], "x", -1)])
    own = [top, column, left, right, far]
    return own + [turn(piece, "c", 1) for piece in own], smalls


def body(token_ids, target_ids, embedding, section_weight, section_gain, final_gain):
    ny, nzh, nc, nzl, nx = (lax.axis_size(a) for a in ("y", "zh", "c", "zl", "x"))
    iy, izh, ic, izl, ix = (lax.axis_index(a) for a in ("y", "zh", "c", "zl", "x"))
    features = embedding.shape[1]
    part_rows = embedding.shape[0]
    vocab_rows = part_rows * nzl * nx
    layers = nzh * nc
    shard = section_weight.shape[1]
    tokens = token_ids.size // layers
    core = jnp.stack([ic, ix])

    vocab_iota = jnp.arange(vocab_rows, dtype=jnp.int32)
    share = izh * nc + ic
    token_own = pick(token_ids.reshape(layers, tokens), share, 0)
    target_own = pick(target_ids.reshape(layers, tokens), share, 0)
    onehot_in = (token_own[:, None] == vocab_iota[None, :]).astype(BF)

    def small(embedding, gain_row):
        gain_pair = in_order(gain_row, turn(gain_row, "c", 1), ic)
        gains = in_order(gain_pair, turn(gain_pair, "zh", 1), izh).reshape(layers, features)
        ring, step = embedding[None], 0
        for axis, count in (("x", nx), ("zl", nzl)):
            reach = 1
            while reach < count:
                step += 1
                ring = jnp.concatenate([ring, turn(ring, axis, reach)])
                reach *= 2
        from_zl = (izl - jnp.arange(nzl)) % nzl
        from_x = (ix - jnp.arange(nx)) % nx
        owner = from_zl[:, None] * nx + from_x[None, :]
        row_ids = (owner[:, :, None] * part_rows + jnp.arange(part_rows)).reshape(-1)
        select = (vocab_iota[:, None] == row_ids[None, :]).astype(BF)
        table = jnp.dot(select, ring.reshape(vocab_rows, features), preferred_element_type=F32).astype(BF)
        return gains, table, jnp.dot(onehot_in, table, preferred_element_type=F32).astype(BF)

    stores, (gains, table, x) = gather_weights(section_weight[0], small, (embedding, section_gain[0]))

    saved = (
        jnp.zeros((layers, tokens, features), BF),
        jnp.zeros((nx, layers, tokens, features // nx), BF),
        jnp.zeros((layers, tokens, features), F32),
        jnp.zeros((layers, tokens, LANES), F32),
        x,
    )
    for stage in range(ny):
        x_in = x if stage == 0 else shift(saved[-1], "y", 1)
        saved = lax.cond(
            iy == stage,
            lambda x_in, saved: tuple(forward_stage(core, x_in, gains, stores, nx)),
            lambda x_in, saved: saved,
            x_in,
            saved,
        )
    xs, ns, slopes, scales, x_top = saved

    q, f, final_part, grad = lax.cond(
        iy == ny - 1,
        lambda x_top: tuple(head_stage(x_top, table, target_own[:, None], final_gain[None, :])),
        lambda x_top: (
            jnp.zeros((tokens, vocab_rows), BF),
            jnp.zeros((tokens, features), BF),
            jnp.zeros((1, features), F32),
            jnp.zeros((tokens, features), BF),
        ),
        x_top,
    )

    pair = layers // nzh

    def backward(stage, grad_in, kept, first, count):
        return lax.cond(
            iy == stage,
            lambda grad_in, kept: tuple(backward_stage(core, grad_in, gains, xs, slopes, scales, stores, first, count)),
            lambda grad_in, kept: kept,
            grad_in,
            kept,
        )

    back = (jnp.zeros((layers, tokens, features), BF), jnp.zeros((layers, features), F32), grad)
    left = jnp.where(iy == 0, onehot_in, q)
    for stage in range(ny - 1, 0, -1):
        grad_in = grad if stage == ny - 1 else shift(back[-1], "y", -1)
        back = backward(stage, grad_in, back, 0, layers)
        if stage == ny - 1:
            back, ns, left = lax.optimization_barrier((back, ns, left))

    n4 = ns.reshape(nx, nzh, nc, tokens, features // nx)
    n_swap = turn(pick(n4, 1 - ic, 2), "c", 1)
    n2 = jnp.stack([pick(n4, ic, 2), n_swap], axis=2)
    left2 = jnp.concatenate([left, turn(left, "c", 1)])

    def columns(to_x):
        return pick(n2, to_x, 0)

    n_parts = [columns(ix)] + [turn(columns((ix + k) % nx), "x", k) for k in (1, -1, 2)]
    n_rows = jnp.transpose(jnp.stack(n_parts, axis=2), (0, 4, 1, 2, 3)).reshape(nzh, nzl * shard, nc * nx * tokens)
    l_rows = pick(left2.reshape(nc * tokens, ny, nzh, nc, nzl, nx), ic, 3)
    l_rows = jnp.transpose(l_rows, (4, 2, 3, 1, 0)).reshape(-1, nc * tokens)

    grad_in = shift(back[-1], "y", -1)
    grad_in, n_rows, l_rows = lax.optimization_barrier((grad_in, n_rows, l_rows))
    last, grad_low = [None] * nzh, grad_in
    for h in range(nzh - 1, -1, -1):
        kept = tuple(b[h * pair : (h + 1) * pair] for b in back[:-1]) + (grad_low,)
        last[h] = backward(0, grad_low, kept, h * pair, pair)
        grad_low = last[h][-1]

    def exchanged(da):
        near = (da, turn(da, "x", 1), turn(da, "x", -1))
        far = jnp.concatenate([turn(near[1][:1], "x", 1), turn(near[2][1:], "x", -1)])
        pieces = jnp.stack(near + (far,))
        return pick(pieces, ic, 1), turn(pick(pieces, 1 - ic, 1), "c", 1)

    das = [None] * nzh
    for h in range(nzh - 1, -1, -1):
        das[h] = exchanged(last[h][0])

    right = jnp.where(iy == 0, grad_low, f)
    gp4 = jnp.stack([last[h][1] for h in range(nzh)])
    misc_rows = 16

    def misc(which):
        return jnp.concatenate(
            [pick(gp4, which, 1), final_part, jnp.zeros((misc_rows - nzh - 1, features), F32)]
        ).astype(BF)

    swapped = turn(jnp.concatenate([right, misc(1 - ic)]), "c", 1)
    right2 = jnp.concatenate([right, swapped[:tokens]])
    rows_all = jnp.dot(l_rows, right2, preferred_element_type=F32).astype(BF).reshape(nx, -1, features)
    misc2 = (misc(ic).astype(F32) + swapped[tokens:].astype(F32)).astype(BF)

    def rows_for(to_x):
        return jnp.concatenate([pick(rows_all, to_x, 0), misc2])

    rows_sum = rows_for(ix).astype(F32)
    for k in (1, -1, 2):
        rows_sum = rows_sum + turn(rows_for((ix + k) % nx), "x", k).astype(F32)
    rows_sum = rows_sum.astype(BF)
    rows_z = rows_sum[: nzh * nzl * ny].reshape(nzh, nzl, ny, features)
    misc_sum = rows_sum[nzh * nzl * ny :]
    gain_rows = jnp.broadcast_to(misc_sum[:nzh].reshape(nzh, 1, 1, features), (nzh, nzl, 1, features))
    final_rows = jnp.broadcast_to(misc_sum[nzh], (nzh, nzl, 1, features))
    extra = 16
    empty = jnp.zeros((nzh, nzl, extra - ny - 2, features), BF)
    tails = jnp.concatenate([rows_z, gain_rows, final_rows, empty], axis=2).reshape(nzh * nzl, extra, features)

    z_axes = ("zh", "zl")
    nz = nzh * nzl
    iz = izh * nzl + izl

    def scattered(blocks, up_steps):
        def block(offset):
            return pick(blocks, (iz + offset) % nz, 0)

        total = block(0).astype(F32)
        for sign, count in ((1, up_steps), (-1, nz - 1 - up_steps)):
            moving = block(sign * count)
            for offset in range(count - 1, 0, -1):
                arrived = turn(moving, z_axes, sign)
                moving = (arrived.astype(F32) + block(sign * offset).astype(F32)).astype(BF)
            total = total + turn(moving, z_axes, sign).astype(F32)
        return total

    chunks = []
    for k in range(COLS):
        flat = [v for pieces in das for v in pieces]
        chunks.append(scattered(product_stage(n_rows, flat, tails, k), nz // 2 - k % 2))
    total = jnp.concatenate(chunks, axis=1)

    weight_grad = total[:shard]
    gain_grad = total[shard + ny : shard + ny + 1]
    rows_y = total[shard : shard + ny]
    final_plane = total[shard + ny + 1 : shard + ny + 2]

    def to_plane(which):
        return jnp.concatenate([pick(rows_y, which, 0)[None], final_plane])

    y_sum = to_plane(iy)
    for k in range(1, ny):
        y_sum = y_sum + turn(to_plane((iy + k) % ny), "y", k)
    return (weight_grad[None], gain_grad, y_sum[:1], y_sum[1])


def solution(mesh):
    names = ("y", "zh", "c", "zl", "x")
    inner = Mesh(mesh.devices.reshape(4, 2, 2, 4, 4), names)
    section = ("y", "zh", "c")
    group = ("zl", "x")
    in_specs = (
        P(None, group),
        P(None, group),
        P(group, None),
        P(section, group, None),
        P(section, None),
        P(),
    )
    out_specs = (
        P(section, group, None),
        P(section, None),
        P(section + group, None),
        P(),
    )
    return jax.shard_map(body, mesh=inner, in_specs=in_specs, out_specs=out_specs, check_vma=False)
```
